8 devices in a mesh: dp: 1 (over z), tp: 8 (over x, y, core).
Axes of the slice: x: 2, y: 2, z: 1, core: 2. Of those that a mesh axis runs over, the one named last changes fastest.
Arguments:
- x: bfloat16 [2048, 3072], P('dp')
- dy: bfloat16 [2048, 3072], P('dp')
- gate: bfloat16 [2048, 8192], P('dp', 'tp')
- up: bfloat16 [2048, 8192], P('dp', 'tp')
- w_gate: bfloat16 [3072, 8192], P(None, 'tp')
- w_up: bfloat16 [3072, 8192], P(None, 'tp')
- w_down: bfloat16 [8192, 3072], P('tp')
Outputs:
- output 1: bfloat16 [2048, 3072], P('dp')
- output 2: bfloat16 [3072, 8192], P('dp', 'tp')
- output 3: bfloat16 [3072, 8192], P('dp', 'tp')
- output 4: bfloat16 [8192, 3072], P(('dp', 'tp'))
All inputs are finite; a program needn't handle non-finite values.
Results may differ from the reference program's by a relative error of at most 0.012.
Values are sent between devices in bfloat16 or wider.
A program may use at most 2 GiB of HBM per device.

```python
import jax
import jax.numpy as jnp

ROWS = 2048
D = 3072
FF = 8192


def act(gate, up):
    return jax.nn.silu(gate) * up


def setup_inputs(seed: int = 0, part: int = 0) -> dict:
    kx, ky, ka, kb, kg, ku, kd = jax.random.split(jax.random.key(seed), 7)
    kx, ky, ka, kb = (jax.random.fold_in(k, part) for k in (kx, ky, ka, kb))
    drawn = {
        "x": jax.random.normal(kx, (ROWS, D), jnp.float32),
        "dy": jax.random.normal(ky, (ROWS, D), jnp.float32),
        "gate": jax.random.normal(ka, (ROWS, FF), jnp.float32),
        "up": jax.random.normal(kb, (ROWS, FF), jnp.float32),
        "w_gate": jax.random.normal(kg, (D, FF), jnp.float32) * D**-0.5,
        "w_up": jax.random.normal(ku, (D, FF), jnp.float32) * D**-0.5,
        "w_down": jax.random.normal(kd, (FF, D), jnp.float32) * FF**-0.5,
    }
    return {k: v.astype(jnp.bfloat16) for k, v in drawn.items()}


def reference(x, dy, gate, up, w_gate, w_up, w_down):
    hidden, back = jax.vjp(act, gate.astype(jnp.float32), up.astype(jnp.float32))
    d_hidden = jnp.dot(dy, w_down.T, preferred_element_type=jnp.float32)
    d_gate, d_up = (g.astype(jnp.bfloat16) for g in back(d_hidden))
    dx = jnp.dot(d_gate, w_gate.T, preferred_element_type=jnp.float32) + jnp.dot(d_up, w_up.T, preferred_element_type=jnp.float32)
    dw_gate = jnp.dot(x.T, d_gate, preferred_element_type=jnp.float32)
    dw_up = jnp.dot(x.T, d_up, preferred_element_type=jnp.float32)
    dw_down = jnp.dot(hidden.astype(jnp.bfloat16).T, dy, preferred_element_type=jnp.float32)
    return tuple(g.astype(jnp.bfloat16) for g in (dx, dw_gate, dw_up, dw_down))
```

```python
import functools

import jax
import jax.numpy as jnp
from jax import lax
from jax.experimental import pallas as pl
from jax.experimental.pallas import tpu as pltpu
from jax.sharding import PartitionSpec as P

BF16, F32 = jnp.bfloat16, jnp.float32
ROWS, D, FL = 2048, 3072, 1024
M = 256
HALF = D // 2
W = 768
PIECES = HALF // W
STEPS = ROWS // M
ANY = pl.BlockSpec(memory_space=pl.ANY)


def nt(a, b):
    return lax.dot_general(a, b, (((1,), (1,)), ((), ())), preferred_element_type=F32)


def place():
    me = lax.axis_index("tp")
    core, y, x = me % 2, (me // 2) % 2, me // 4
    return me, core, y, x


def rows_of(p, x, y):
    diag, own = 1 - jnp.minimum(p // 2, 1), p // 6
    mid = 1 - diag - own
    block = diag * p + own * (p - 6) + mid * ((p - 2) // 2)
    flip_x = diag + mid * (p % 2)
    flip_y = diag + mid * (1 - p % 2)
    to_x = x + flip_x - 2 * x * flip_x
    to_y = y + flip_y - 2 * y * flip_y
    return ((to_x * 2 + to_y) * 2 + block) * M, diag, mid, own, block


def scatter_kernel(
    dy, gate, up, w_gate, w_up, w_down,
    shard, d_gate, d_up, hidden,
    wg, wu, wd, dyb, gb, ub, dgb, dub, hb, acc, sum_own, done,
    sib_out, sib_in, one_out, one_in, two_out, two_in,
    w_sem, in_sem, out_sem, done_sem,
    sib_s, sib_r, one_s, one_r, two_s, two_r,
):
    me, core, y, x = place()
    sibling = me + 1 - 2 * core
    near_x, near_y = me + 4 - 8 * x, me + 2 - 4 * y
    first = near_y * (1 - core) + near_x * core
    second = near_x * (1 - core) + near_y * core
    own_col, sib_col = core * HALF, (1 - core) * HALF

    def inputs(p, slot):
        row = rows_of(p, x, y)[0]
        rows = pl.ds(pl.multiple_of(row, M), M)
        return [
            pltpu.make_async_copy(dy.at[rows], dyb.at[slot], in_sem.at[slot, 0]),
            pltpu.make_async_copy(gate.at[rows], gb.at[slot], in_sem.at[slot, 1]),
            pltpu.make_async_copy(up.at[rows], ub.at[slot], in_sem.at[slot, 2]),
        ]

    def outputs(p, slot):
        row = rows_of(p, x, y)[0]
        rows = pl.ds(pl.multiple_of(row, M), M)
        return [
            pltpu.make_async_copy(dgb.at[slot], d_gate.at[rows], out_sem.at[slot, 0]),
            pltpu.make_async_copy(dub.at[slot], d_up.at[rows], out_sem.at[slot, 1]),
            pltpu.make_async_copy(hb.at[slot], hidden.at[rows], out_sem.at[slot, 2]),
        ]

    def columns(base, j):
        return pl.ds(pl.multiple_of(base + j * W, 256), W)

    down = pltpu.make_async_copy(w_down, wd, w_sem.at[0])
    wide = []
    for k, (base, j) in enumerate([(b, j) for b in (sib_col, own_col) for j in range(PIECES)]):
        at = columns(base, j)
        wide.append(pltpu.make_async_copy(w_gate.at[at], wg.at[at], w_sem.at[1 + 2 * k]))
        wide.append(pltpu.make_async_copy(w_up.at[at], wu.at[at], w_sem.at[2 + 2 * k]))

    def remote(src, dst, send, recv, to):
        return pltpu.make_async_remote_copy(
            src_ref=src, dst_ref=dst, send_sem=send, recv_sem=recv,
            device_id={"tp": to}, device_id_type=pl.DeviceIdType.MESH,
        )

    def to_sibling(p, j):
        return remote(sib_out.at[p, j], sib_in.at[p, j], sib_s.at[p, j], sib_r.at[p, j], sibling)

    def to_first(k, j):
        return remote(one_out.at[k, j], one_in.at[k, j], one_s.at[k, j], one_r.at[k, j], first)

    def to_second(k, j):
        return remote(two_out.at[k, j], two_in.at[k, j], two_s.at[k, j], two_r.at[k, j], second)

    for c in inputs(0, 0):
        c.start()
    down.start()
    for c in wide:
        c.start()

    barrier = pltpu.get_barrier_semaphore()
    for other in (sibling, first, second):
        pl.semaphore_signal(barrier, inc=1, device_id={"tp": other}, device_id_type=pl.DeviceIdType.MESH)
    pl.semaphore_wait(barrier, 3)

    def step(p, carry):
        slot = p % 2
        _, diag, mid, own, block = rows_of(p, x, y)
        is_first = diag + mid * (1 - (p + core) % 2)
        is_second = mid * ((p + core) % 2)
        for c in inputs(p, slot):
            c.wait()

        @pl.when(p < STEPS - 1)
        def _():
            for c in inputs(p + 1, 1 - slot):
                c.start()

        @pl.when(p >= 2)
        def _():
            for c in outputs(p - 2, slot):
                c.wait()

        @pl.when(p == 0)
        def _():
            down.wait()

        for n in range(FL // 256):
            at = slice(n * 256, (n + 1) * 256)
            d_hidden = nt(dyb[slot], wd[at, :])
            g, u = gb[slot, :, at].astype(F32), ub[slot, :, at].astype(F32)
            s = jax.nn.sigmoid(g)
            act = g * s
            hb[slot, :, at] = (act * u).astype(BF16)
            dub[slot, :, at] = (d_hidden * act).astype(BF16)
            dgb[slot, :, at] = (d_hidden * u * (s + act * (1 - s))).astype(BF16)
        for c in outputs(p, slot):
            c.start()

        @pl.when(p == 0)
        def _():
            for c in wide:
                c.wait()

        for j in range(PIECES):
            at = columns(sib_col, j)
            sib_out[p, j] = (nt(dgb[slot], wg[at, :]) + nt(dub[slot], wu[at, :])).astype(BF16)
            to_sibling(p, j).start()
        for j in range(PIECES):
            at = columns(own_col, j)
            acc[j] = nt(dgb[slot], wg[at, :]) + nt(dub[slot], wu[at, :])
        for j in range(PIECES):
            to_sibling(p, j).wait_recv()

            @pl.when(is_first == 1)
            def _():
                k = diag * block + mid * (2 + block)
                one_out[k, j] = (acc[j] + sib_in[p, j].astype(F32)).astype(BF16)
                to_first(k, j).start()

            @pl.when(is_second == 1)
            def _():
                to_first(block, j).wait_recv()
                two_out[block, j] = (acc[j] + sib_in[p, j].astype(F32) + one_in[block, j].astype(F32)).astype(BF16)
                to_second(block, j).start()

            @pl.when(own == 1)
            def _():
                sum_own[block, j] = acc[j] + sib_in[p, j].astype(F32)

        return carry

    lax.fori_loop(0, STEPS, step, 0)

    stores = []
    for b in range(2):
        for j in range(PIECES):
            to_first(2 + b, j).wait_recv()
            to_second(b, j).wait_recv()
            done[b, j] = (sum_own[b, j] + one_in[2 + b, j].astype(F32) + two_in[b, j].astype(F32)).astype(BF16)
            stores.append(
                pltpu.make_async_copy(
                    done.at[b, j], shard.at[pl.ds(b * M, M), pl.ds(j * W, W)], done_sem.at[b, j]
                )
            )
            stores[-1].start()
    for p in (STEPS - 2, STEPS - 1):
        for c in outputs(p, p % 2):
            c.wait()
    for j in range(PIECES):
        for p in range(STEPS):
            to_sibling(p, j).wait_send()
        for k in range(4):
            to_first(k, j).wait_send()
        for k in range(2):
            to_second(k, j).wait_send()
    for c in stores:
        c.wait()


def scatter(dy, gate, up, w_gate, w_up, w_down):
    dma = pltpu.SemaphoreType.DMA
    hid = jax.ShapeDtypeStruct((ROWS, FL), BF16)
    piece = lambda n: pltpu.VMEM((n, PIECES, M, W), BF16)
    return pl.pallas_call(
        scatter_kernel,
        out_shape=(jax.ShapeDtypeStruct((2 * M, HALF), BF16), hid, hid, hid),
        in_specs=[ANY] * 6,
        out_specs=(ANY,) * 4,
        scratch_shapes=[
            pltpu.VMEM((D, FL), BF16), pltpu.VMEM((D, FL), BF16), pltpu.VMEM((FL, D), BF16),
            pltpu.VMEM((2, M, D), BF16), pltpu.VMEM((2, M, FL), BF16), pltpu.VMEM((2, M, FL), BF16),
            pltpu.VMEM((2, M, FL), BF16), pltpu.VMEM((2, M, FL), BF16), pltpu.VMEM((2, M, FL), BF16),
            pltpu.VMEM((PIECES, M, W), F32), pltpu.VMEM((2, PIECES, M, W), F32), piece(2),
            piece(STEPS), piece(STEPS), piece(4), piece(4), piece(2), piece(2),
            dma((1 + 4 * PIECES,)), dma((2, 3)), dma((2, 3)), dma((2, PIECES)),
            dma((STEPS, PIECES)), dma((STEPS, PIECES)), dma((4, PIECES)), dma((4, PIECES)),
            dma((2, PIECES)), dma((2, PIECES)),
        ],
        compiler_params=pltpu.CompilerParams(
            collective_id=0, has_side_effects=True, vmem_limit_bytes=63 * 1024 * 1024
        ),
        cost_estimate=pl.CostEstimate(
            flops=6 * 2 * ROWS * D * FL // 2, bytes_accessed=60 * 2**20, transcendentals=2 * ROWS * FL
        ),
        name="scatter",
    )(dy, gate, up, w_gate, w_up, w_down)


def turned(a, b):
    return lax.dot_general(a, b, (((0,), (0,)), ((), ())), preferred_element_type=F32)


def wide_kernel(x, d_gate, d_up, dw_gate, dw_up, xt):
    xt[...] = x[...].T
    dw_gate[...] = jnp.dot(xt[...], d_gate[...], preferred_element_type=F32).astype(BF16)
    dw_up[...] = jnp.dot(xt[...], d_up[...], preferred_element_type=F32).astype(BF16)


def wide_grads(x, d_gate, d_up, bm=512):
    whole = pl.BlockSpec((ROWS, FL), lambda i: (0, 0))
    out = pl.BlockSpec((bm, FL), lambda i: (i, 0))
    shape = jax.ShapeDtypeStruct((D, FL), BF16)
    return pl.pallas_call(
        wide_kernel,
        grid=(D // bm,),
        out_shape=(shape, shape),
        in_specs=[pl.BlockSpec((ROWS, bm), lambda i: (0, i)), whole, whole],
        out_specs=(out, out),
        scratch_shapes=[pltpu.VMEM((bm, ROWS), BF16)],
        compiler_params=pltpu.CompilerParams(vmem_limit_bytes=50 * 1024 * 1024),
        cost_estimate=pl.CostEstimate(flops=4 * ROWS * D * FL, bytes_accessed=34 * 2**20, transcendentals=0),
        name="wide_grads",
    )(x, d_gate, d_up)


def down_kernel(hidden, dy, out, ht):
    @pl.when(pl.program_id(0) == 0)
    def _():
        ht[...] = hidden[...].T

    out[...] = jnp.dot(ht[...], dy[...], preferred_element_type=F32).astype(BF16)


def down_grad(hidden, dy, bn=512):
    return pl.pallas_call(
        down_kernel,
        grid=(D // bn,),
        out_shape=jax.ShapeDtypeStruct((FL, D), BF16),
        in_specs=[pl.BlockSpec((ROWS, FL), lambda i: (0, 0)), pl.BlockSpec((ROWS, bn), lambda i: (0, i))],
        out_specs=pl.BlockSpec((FL, bn), lambda i: (0, i)),
        scratch_shapes=[pltpu.VMEM((FL, ROWS), BF16)],
        compiler_params=pltpu.CompilerParams(vmem_limit_bytes=50 * 1024 * 1024),
        cost_estimate=pl.CostEstimate(flops=2 * ROWS * D * FL, bytes_accessed=24 * 2**20, transcendentals=0),
        name="down_grad",
    )(hidden, dy)


def assemble_kernel(*refs):
    parts, out, buf, in_sem, out_sem = refs[:8], refs[8], refs[9], refs[10], refs[11]
    me, core, y, x = place()
    reads, writes = [], []
    for k in range(8):
        c, f, s = k % 2, (k // 2) % 2, k // 4
        half = core + c - 2 * core * c
        flip_y = f * (1 - half) + s * half
        flip_x = f * half + s * (1 - half)
        to_x, to_y = x + flip_x - 2 * x * flip_x, y + flip_y - 2 * y * flip_y
        rows = pl.ds(pl.multiple_of((to_x * 2 + to_y) * 2 * M, 2 * M), 2 * M)
        cols = pl.ds(pl.multiple_of(half * HALF, HALF), HALF)
        reads.append(pltpu.make_async_copy(parts[k], buf.at[k], in_sem.at[k]))
        writes.append(pltpu.make_async_copy(buf.at[k], out.at[rows, cols], out_sem.at[k]))
    for c in reads:
        c.start()
    for r, w in zip(reads, writes):
        r.wait()
        w.start()
    for c in writes:
        c.wait()


def assemble(parts):
    return pl.pallas_call(
        assemble_kernel,
        out_shape=jax.ShapeDtypeStruct((ROWS, D), BF16),
        in_specs=[ANY] * 8,
        out_specs=ANY,
        scratch_shapes=[
            pltpu.VMEM((8, 2 * M, HALF), BF16), pltpu.SemaphoreType.DMA((8,)), pltpu.SemaphoreType.DMA((8,)),
        ],
        compiler_params=pltpu.CompilerParams(vmem_limit_bytes=20 * 1024 * 1024),
        cost_estimate=pl.CostEstimate(flops=10**9, bytes_accessed=24 * 2**20, transcendentals=0),
        name="assemble",
    )(*parts)


def index(x, y, core):
    return (x * 2 + y) * 2 + core


def pairs(to):
    return [(index(x, y, c), index(*to(x, y, c))) for x in (0, 1) for y in (0, 1) for c in (0, 1)]


FIRST = pairs(lambda x, y, c: (x, 1 - y, c) if c == 0 else (1 - x, y, c))
SECOND = pairs(lambda x, y, c: (1 - x, y, c) if c == 0 else (x, 1 - y, c))
SIBLING = pairs(lambda x, y, c: (x, y, 1 - c))


def solution(mesh):
    def step(x, dy, gate, up, w_gate, w_up, w_down):
        shard, d_gate, d_up, hidden = scatter(dy, gate, up, w_gate, w_up, w_down)
        send = functools.partial(lax.ppermute, axis_name="tp")
        from_first, from_second = send(shard, perm=FIRST), send(shard, perm=SECOND)
        own_twin = send(shard, perm=SIBLING)
        from_both = send(from_first, perm=SECOND)
        first_twin, second_twin = send(from_first, perm=SIBLING), send(from_second, perm=SIBLING)
        both_twin = send(from_both, perm=SIBLING)
        dw_gate, dw_up = wide_grads(x, d_gate, d_up)
        dw_down = down_grad(hidden, dy)
        dx = assemble(
            (shard, own_twin, from_first, first_twin, from_second, second_twin, from_both, both_twin)
        )
        return dx, dw_gate, dw_up, dw_down

    tokens, columns, rows = P("dp", None), P(None, "tp"), P("tp", None)
    return jax.shard_map(
        step,
        mesh=mesh,
        in_specs=(tokens, tokens, P("dp", "tp"), P("dp", "tp"), columns, columns, rows),
        out_specs=(tokens, P("dp", "tp"), P("dp", "tp"), P(("dp", "tp"), None)),
        check_vma=False,
    )
```

```python
import jax
import jax.numpy as jnp
from jax import lax
from jax.experimental import pallas as pl
from jax.experimental.pallas import tpu as pltpu
from jax.sharding import PartitionSpec as P


BF16, F32 = jnp.bfloat16, jnp.float32
ROWS, D, FL = 2048, 3072, 1024
M = 256
HALF = D // 2
W = 768
PIECES = HALF // W
STEPS = ROWS // M
ANY = pl.BlockSpec(memory_space=pl.ANY)


def nt(a, b):
    return lax.dot_general(a, b, (((1,), (1,)), ((), ())), preferred_element_type=F32)


def place():
    me = lax.axis_index("tp")
    core, y, x = me % 2, (me // 2) % 2, me // 4
    return me, core, y, x


def rows_of(p, x, y):
    diag, own = 1 - jnp.minimum(p // 2, 1), p // 6
    mid = 1 - diag - own
    block = diag * p + own * (p - 6) + mid * ((p - 2) // 2)
    flip_x = diag + mid * (p % 2)
    flip_y = diag + mid * (1 - p % 2)
    to_x = x + flip_x - 2 * x * flip_x
    to_y = y + flip_y - 2 * y * flip_y
    return ((to_x * 2 + to_y) * 2 + block) * M, diag, mid, own, block


def scatter_kernel(
    dy, gate, up, w_gate, w_up, w_down,
    shard, d_gate, d_up, hidden,
    wg, wu, wd, dyb, gb, ub, dgb, dub, hb, acc, sum_own, done,
    sib_out, sib_in, one_out, one_in, two_out, two_in,
    w_sem, in_sem, out_sem, done_sem,
    sib_s, sib_r, one_s, one_r, two_s, two_r,
):
    me, core, y, x = place()
    sibling = me + 1 - 2 * core
    near_x, near_y = me + 4 - 8 * x, me + 2 - 4 * y
    first = near_y * (1 - core) + near_x * core
    second = near_x * (1 - core) + near_y * core
    own_col, sib_col = core * HALF, (1 - core) * HALF

    def inputs(p, slot):
        row = rows_of(p, x, y)[0]
        rows = pl.ds(pl.multiple_of(row, M), M)
        return [
            pltpu.make_async_copy(dy.at[rows], dyb.at[slot], in_sem.at[slot, 0]),
            pltpu.make_async_copy(gate.at[rows], gb.at[slot], in_sem.at[slot, 1]),
            pltpu.make_async_copy(up.at[rows], ub.at[slot], in_sem.at[slot, 2]),
        ]

    def outputs(p, slot):
        row = rows_of(p, x, y)[0]
        rows = pl.ds(pl.multiple_of(row, M), M)
        return [
            pltpu.make_async_copy(dgb.at[slot], d_gate.at[rows], out_sem.at[slot, 0]),
            pltpu.make_async_copy(dub.at[slot], d_up.at[rows], out_sem.at[slot, 1]),
            pltpu.make_async_copy(hb.at[slot], hidden.at[rows], out_sem.at[slot, 2]),
        ]

    def columns(base, j):
        return pl.ds(pl.multiple_of(base + j * W, 256), W)

    down = pltpu.make_async_copy(w_down, wd, w_sem.at[0])
    wide = []
    for k, (base, j) in enumerate([(b, j) for b in (sib_col, own_col) for j in range(PIECES)]):
        at = columns(base, j)
        wide.append(pltpu.make_async_copy(w_gate.at[at], wg.at[at], w_sem.at[1 + 2 * k]))
        wide.append(pltpu.make_async_copy(w_up.at[at], wu.at[at], w_sem.at[2 + 2 * k]))

    def remote(src, dst, send, recv, to):
        return pltpu.make_async_remote_copy(
            src_ref=src, dst_ref=dst, send_sem=send, recv_sem=recv,
            device_id={"tp": to}, device_id_type=pl.DeviceIdType.MESH,
        )

    def to_sibling(p, j):
        return remote(sib_out.at[p, j], sib_in.at[p, j], sib_s.at[p, j], sib_r.at[p, j], sibling)

    def to_first(k, j):
        return remote(one_out.at[k, j], one_in.at[k, j], one_s.at[k, j], one_r.at[k, j], first)

    def to_second(k, j):
        return remote(two_out.at[k, j], two_in.at[k, j], two_s.at[k, j], two_r.at[k, j], second)

    for c in inputs(0, 0):
        c.start()
    down.start()
    for c in wide:
        c.start()

    barrier = pltpu.get_barrier_semaphore()
    for other in (sibling, first, second):
        pl.semaphore_signal(barrier, inc=1, device_id={"tp": other}, device_id_type=pl.DeviceIdType.MESH)
    pl.semaphore_wait(barrier, 3)

    def step(p, carry):
        slot = p % 2
        _, diag, mid, own, block = rows_of(p, x, y)
        is_first = diag + mid * (1 - (p + core) % 2)
        is_second = mid * ((p + core) % 2)
        for c in inputs(p, slot):
            c.wait()

        @pl.when(p < STEPS - 1)
        def _():
            for c in inputs(p + 1, 1 - slot):
                c.start()

        @pl.when(p >= 2)
        def _():
            for c in outputs(p - 2, slot):
                c.wait()

        @pl.when(p == 0)
        def _():
            down.wait()

        for n in range(FL // 256):
            at = slice(n * 256, (n + 1) * 256)
            d_hidden = nt(dyb[slot], wd[at, :])
            g, u = gb[slot, :, at].astype(F32), ub[slot, :, at].astype(F32)
            s = jax.nn.sigmoid(g)
            act = g * s
            hb[slot, :, at] = (act * u).astype(BF16)
            dub[slot, :, at] = (d_hidden * act).astype(BF16)
            dgb[slot, :, at] = (d_hidden * u * (s + act * (1 - s))).astype(BF16)
        for c in outputs(p, slot):
            c.start()

        @pl.when(p == 0)
        def _():
            for c in wide:
                c.wait()

        for j in range(PIECES):
            at = columns(sib_col, j)
            sib_out[p, j] = (nt(dgb[slot], wg[at, :]) + nt(dub[slot], wu[at, :])).astype(BF16)
            to_sibling(p, j).start()
        for j in range(PIECES):
            at = columns(own_col, j)
            acc[j] = nt(dgb[slot], wg[at, :]) + nt(dub[slot], wu[at, :])
        for j in range(PIECES):
            to_sibling(p, j).wait_recv()

            @pl.when(is_first == 1)
            def _():
                k = diag * block + mid * (2 + block)
                one_out[k, j] = (acc[j] + sib_in[p, j].astype(F32)).astype(BF16)
                to_first(k, j).start()

            @pl.when(is_second == 1)
            def _():
                to_first(block, j).wait_recv()
                two_out[block, j] = (acc[j] + sib_in[p, j].astype(F32) + one_in[block, j].astype(F32)).astype(BF16)
                to_second(block, j).start()

            @pl.when(own == 1)
            def _():
                sum_own[block, j] = acc[j] + sib_in[p, j].astype(F32)

        return carry

    lax.fori_loop(0, STEPS, step, 0)

    stores = []
    for b in range(2):
        for j in range(PIECES):
            to_first(2 + b, j).wait_recv()
            to_second(b, j).wait_recv()
            done[b, j] = (sum_own[b, j] + one_in[2 + b, j].astype(F32) + two_in[b, j].astype(F32)).astype(BF16)
            stores.append(
                pltpu.make_async_copy(
                    done.at[b, j], shard.at[pl.ds(b * M, M), pl.ds(j * W, W)], done_sem.at[b, j]
                )
            )
            stores[-1].start()
    for p in (STEPS - 2, STEPS - 1):
        for c in outputs(p, p % 2):
            c.wait()
    for j in range(PIECES):
        for p in range(STEPS):
            to_sibling(p, j).wait_send()
        for k in range(4):
            to_first(k, j).wait_send()
        for k in range(2):
            to_second(k, j).wait_send()
    for c in stores:
        c.wait()


def scatter(dy, gate, up, w_gate, w_up, w_down):
    dma = pltpu.SemaphoreType.DMA
    hid = jax.ShapeDtypeStruct((ROWS, FL), BF16)
    piece = lambda n: pltpu.VMEM((n, PIECES, M, W), BF16)
    return pl.pallas_call(
        scatter_kernel,
        out_shape=(jax.ShapeDtypeStruct((2 * M, HALF), BF16), hid, hid, hid),
        in_specs=[ANY] * 6,
        out_specs=(ANY,) * 4,
        scratch_shapes=[
            pltpu.VMEM((D, FL), BF16), pltpu.VMEM((D, FL), BF16), pltpu.VMEM((FL, D), BF16),
            pltpu.VMEM((2, M, D), BF16), pltpu.VMEM((2, M, FL), BF16), pltpu.VMEM((2, M, FL), BF16),
            pltpu.VMEM((2, M, FL), BF16), pltpu.VMEM((2, M, FL), BF16), pltpu.VMEM((2, M, FL), BF16),
            pltpu.VMEM((PIECES, M, W), F32), pltpu.VMEM((2, PIECES, M, W), F32), piece(2),
            piece(STEPS), piece(STEPS), piece(4), piece(4), piece(2), piece(2),
            dma((1 + 4 * PIECES,)), dma((2, 3)), dma((2, 3)), dma((2, PIECES)),
            dma((STEPS, PIECES)), dma((STEPS, PIECES)), dma((4, PIECES)), dma((4, PIECES)),
            dma((2, PIECES)), dma((2, PIECES)),
        ],
        compiler_params=pltpu.CompilerParams(
            collective_id=0, has_side_effects=True, vmem_limit_bytes=63 * 1024 * 1024
        ),
        cost_estimate=pl.CostEstimate(
            flops=6 * 2 * ROWS * D * FL // 2, bytes_accessed=60 * 2**20, transcendentals=2 * ROWS * FL
        ),
        name="scatter",
    )(dy, gate, up, w_gate, w_up, w_down)


def wide_kernel(x, d_gate, d_up, dw_gate, dw_up, xt):
    xt[...] = x[...].T
    dw_gate[...] = jnp.dot(xt[...], d_gate[...], preferred_element_type=F32).astype(BF16)
    dw_up[...] = jnp.dot(xt[...], d_up[...], preferred_element_type=F32).astype(BF16)


def wide_grads(x, d_gate, d_up, bm=512):
    whole = pl.BlockSpec((ROWS, FL), lambda i: (0, 0))
    out = pl.BlockSpec((bm, FL), lambda i: (i, 0))
    shape = jax.ShapeDtypeStruct((D, FL), BF16)
    return pl.pallas_call(
        wide_kernel,
        grid=(D // bm,),
        out_shape=(shape, shape),
        in_specs=[pl.BlockSpec((ROWS, bm), lambda i: (0, i)), whole, whole],
        out_specs=(out, out),
        scratch_shapes=[pltpu.VMEM((bm, ROWS), BF16)],
        compiler_params=pltpu.CompilerParams(vmem_limit_bytes=50 * 1024 * 1024),
        cost_estimate=pl.CostEstimate(flops=4 * ROWS * D * FL, bytes_accessed=34 * 2**20, transcendentals=0),
        name="wide_grads",
    )(x, d_gate, d_up)


def down_kernel(hidden, dy, out, ht):
    @pl.when(pl.program_id(0) == 0)
    def _():
        ht[...] = hidden[...].T

    out[...] = jnp.dot(ht[...], dy[...], preferred_element_type=F32).astype(BF16)


def down_grad(hidden, dy, bn=512):
    return pl.pallas_call(
        down_kernel,
        grid=(D // bn,),
        out_shape=jax.ShapeDtypeStruct((FL, D), BF16),
        in_specs=[pl.BlockSpec((ROWS, FL), lambda i: (0, 0)), pl.BlockSpec((ROWS, bn), lambda i: (0, i))],
        out_specs=pl.BlockSpec((FL, bn), lambda i: (0, i)),
        scratch_shapes=[pltpu.VMEM((FL, ROWS), BF16)],
        compiler_params=pltpu.CompilerParams(vmem_limit_bytes=50 * 1024 * 1024),
        cost_estimate=pl.CostEstimate(flops=2 * ROWS * D * FL, bytes_accessed=24 * 2**20, transcendentals=0),
        name="down_grad",
    )(hidden, dy)


def assemble_kernel(*refs):
    parts, out, buf, in_sem, out_sem = refs[:8], refs[8], refs[9], refs[10], refs[11]
    _, core, y, x = place()
    reads, writes = [], []
    for k in range(8):
        c, f, s = k % 2, (k // 2) % 2, k // 4
        half = core + c - 2 * core * c
        flip_y = f * (1 - half) + s * half
        flip_x = f * half + s * (1 - half)
        to_x, to_y = x + flip_x - 2 * x * flip_x, y + flip_y - 2 * y * flip_y
        rows = pl.ds(pl.multiple_of((to_x * 2 + to_y) * 2 * M, 2 * M), 2 * M)
        cols = pl.ds(pl.multiple_of(half * HALF, HALF), HALF)
        reads.append(pltpu.make_async_copy(parts[k], buf.at[k], in_sem.at[k]))
        writes.append(pltpu.make_async_copy(buf.at[k], out.at[rows, cols], out_sem.at[k]))
    for c in reads:
        c.start()
    for r, w in zip(reads, writes):
        r.wait()
        w.start()
    for c in writes:
        c.wait()


def assemble(parts):
    return pl.pallas_call(
        assemble_kernel,
        out_shape=jax.ShapeDtypeStruct((ROWS, D), BF16),
        in_specs=[ANY] * 8,
        out_specs=ANY,
        scratch_shapes=[
            pltpu.VMEM((8, 2 * M, HALF), BF16), pltpu.SemaphoreType.DMA((8,)), pltpu.SemaphoreType.DMA((8,)),
        ],
        compiler_params=pltpu.CompilerParams(vmem_limit_bytes=20 * 1024 * 1024),
        cost_estimate=pl.CostEstimate(flops=10**9, bytes_accessed=24 * 2**20, transcendentals=0),
        name="assemble",
    )(*parts)


def index(x, y, core):
    return (x * 2 + y) * 2 + core


def pairs(to):
    return [(index(x, y, c), index(*to(x, y, c))) for x in (0, 1) for y in (0, 1) for c in (0, 1)]


FIRST = pairs(lambda x, y, c: (x, 1 - y, c) if c == 0 else (1 - x, y, c))
SECOND = pairs(lambda x, y, c: (1 - x, y, c) if c == 0 else (x, 1 - y, c))
SIBLING = pairs(lambda x, y, c: (x, y, 1 - c))


def solution(mesh):
    def send(value, perm):
        return lax.ppermute(value, "tp", perm)

    def step(x, dy, gate, up, w_gate, w_up, w_down):
        shard, d_gate, d_up, hidden = scatter(dy, gate, up, w_gate, w_up, w_down)
        from_first, from_second = send(shard, FIRST), send(shard, SECOND)
        own_twin = send(shard, SIBLING)
        from_both = send(from_first, SECOND)
        first_twin = send(from_first, SIBLING)
        second_twin = send(from_second, SIBLING)
        both_twin = send(from_both, SIBLING)
        dw_gate, dw_up = wide_grads(x, d_gate, d_up)
        dw_down = down_grad(hidden, dy)
        dx = assemble(
            (shard, own_twin, from_first, first_twin, from_second, second_twin, from_both, both_twin)
        )
        return dx, dw_gate, dw_up, dw_down

    tokens, columns, rows = P("dp", None), P(None, "tp"), P("tp", None)
    return jax.shard_map(
        step,
        mesh=mesh,
        in_specs=(tokens, tokens, P("dp", "tp"), P("dp", "tp"), columns, columns, rows),
        out_specs=(tokens, P("dp", "tp"), P("dp", "tp"), P(("dp", "tp"), None)),
        check_vma=False,
    )
```

```python
import functools

import jax
import jax.numpy as jnp
from jax import lax
from jax.experimental import pallas as pl
from jax.experimental.pallas import tpu as pltpu
from jax.sharding import PartitionSpec as P


BF16, F32 = jnp.bfloat16, jnp.float32
ROWS, D, FL = 2048, 3072, 1024
M = 256
U = M // 2
HALF = D // 2
W = 512
PIECES = HALF // W
STEPS = ROWS // M
ANY = pl.BlockSpec(memory_space=pl.ANY)


def nt(a, b):
    return lax.dot_general(a, b, (((1,), (1,)), ((), ())), preferred_element_type=F32)


def place():
    me = lax.axis_index("tp")
    core, y, x = me % 2, (me // 2) % 2, me // 4
    return me, core, y, x


def rows_of(p, x, y):
    diag, own = 1 - jnp.minimum(p // 2, 1), p // 6
    mid = 1 - diag - own
    at = diag * p * M + own * (p - 6) * M + mid * (p - 2) * U

    def run(flip_x, flip_y):
        to_x, to_y = x + flip_x - 2 * x * flip_x, y + flip_y - 2 * y * flip_y
        return (to_x * 2 + to_y) * 2 * M + at

    return run(diag, diag + mid), run(diag + mid, diag) + (1 - mid) * U


def scatter_kernel(
    dy, gate, up, w_gate, w_up, w_down,
    shard, d_gate, d_up, hidden,
    wg, wu, wd, dyb, gb, ub, dgb, dub, hb, acc, sum_own, done,
    sib_out, sib_in, one_out, one_in, two_out, two_in,
    down_sem, wide_sem, in_sem, out_sem, done_sem,
    sib_s, sib_r, one_s, one_r, two_s, two_r,
):
    me, core, y, x = place()
    sibling = me + 1 - 2 * core
    near_x, near_y = me + 4 - 8 * x, me + 2 - 4 * y
    first = near_y * (1 - core) + near_x * core
    second = near_x * (1 - core) + near_y * core
    own_col, sib_col = core * HALF, (1 - core) * HALF

    def copies(p, slot, outward):
        made = []
        arrays = ((dgb, d_gate), (dub, d_up), (hb, hidden)) if outward else ((dyb, dy), (gb, gate), (ub, up))
        for h, row in enumerate(rows_of(p, x, y)):
            rows = pl.ds(pl.multiple_of(row, U), U)
            for k, (near, far) in enumerate(arrays):
                near, far = near.at[slot, pl.ds(h * U, U)], far.at[rows]
                if outward:
                    made.append(pltpu.make_async_copy(near, far, out_sem.at[slot, h, k]))
                else:
                    made.append(pltpu.make_async_copy(far, near, in_sem.at[slot, h, k]))
        return made

    def columns(base, j):
        return pl.ds(pl.multiple_of(base + j * W, 256), W)

    down = []
    for n in range(FL // 256):
        at = pl.ds(n * 256, 256)
        down.append(pltpu.make_async_copy(w_down.at[at], wd.at[at], down_sem.at[n]))
    wide = {}
    for j in range(PIECES):
        for side, base in ((0, sib_col), (1, own_col)):
            at = columns(base, j)
            wide[side, j] = (
                pltpu.make_async_copy(w_gate.at[at], wg.at[at], wide_sem.at[side, j, 0]),
                pltpu.make_async_copy(w_up.at[at], wu.at[at], wide_sem.at[side, j, 1]),
            )

    def remote(src, dst, send, recv, to):
        return pltpu.make_async_remote_copy(
            src_ref=src, dst_ref=dst, send_sem=send, recv_sem=recv,
            device_id={"tp": to}, device_id_type=pl.DeviceIdType.MESH,
        )

    def to_sibling(p, j):
        return remote(sib_out.at[p, j], sib_in.at[p, j], sib_s, sib_r.at[p, j], sibling)

    def to_first(k, j):
        return remote(one_out.at[k, j], one_in.at[k, j], one_s, one_r.at[k, j], first)

    def to_second(k, j):
        return remote(two_out.at[k, j], two_in.at[k, j], two_s, two_r.at[k, j], second)

    for c in copies(0, 0, False):
        c.start()
    for c in down:
        c.start()

    barrier = pltpu.get_barrier_semaphore()
    for other in (sibling, first, second):
        pl.semaphore_signal(barrier, inc=1, device_id={"tp": other}, device_id_type=pl.DeviceIdType.MESH)
    pl.semaphore_wait(barrier, 3)

    def hidden_grads(slot, n):
        at = slice(n * 256, (n + 1) * 256)
        d_hidden = nt(dyb[slot], wd[at, :])
        g, u = gb[slot, :, at].astype(F32), ub[slot, :, at].astype(F32)
        s = jax.nn.sigmoid(g)
        act = g * s
        hb[slot, :, at] = (act * u).astype(BF16)
        dub[slot, :, at] = (d_hidden * act).astype(BF16)
        dgb[slot, :, at] = (d_hidden * u * (s + act * (1 - s))).astype(BF16)

    def term(slot, base, j):
        at = columns(base, j)
        return (nt(dgb[slot], wg[at, :]) + nt(dub[slot], wu[at, :])).reshape(2, U, W)

    def for_sibling(p, slot, j):
        sib_out[p, j] = term(slot, sib_col, j).astype(BF16)
        to_sibling(p, j).start()

    def chip_sum(p, j, h):
        return acc[j, h] + sib_in[p, j, h].astype(F32)

    def send_diagonal(p, j):
        for h in range(2):
            one_out[2 * p + h, j] = chip_sum(p, j, h).astype(BF16)
            to_first(2 * p + h, j).start()

    def send_middle(p):
        q = p - 2
        for j in range(PIECES):
            to_sibling(p, j).wait_recv()
            one_out[4 + q, j] = chip_sum(p, j, core).astype(BF16)
            to_first(4 + q, j).start()
        for j in range(PIECES):
            to_first(q, j).wait_recv()
            two_out[q, j] = (chip_sum(p, j, 1 - core) + one_in[q, j].astype(F32)).astype(BF16)
            to_second(q, j).start()

    def keep_own(p):
        for j in range(PIECES):
            to_sibling(p, j).wait_recv()
            for h in range(2):
                sum_own[2 * (p - 6) + h, j] = chip_sum(p, j, h)

    def diagonal_step(p, ready):
        for n in range(FL // 256):
            hidden_grads(p, n)
        for c in copies(p, p, True):
            c.start()
        for j in range(PIECES + 1):
            if j < PIECES:
                ready(0, j)
                for_sibling(p, p, j)
            if j:
                ready(1, j - 1)
                acc[j - 1] = term(p, own_col, j - 1)
                to_sibling(p, j - 1).wait_recv()
                send_diagonal(p, j - 1)

    def arrived(side, j):
        for c in wide[side, j]:
            c.wait()

    for c in copies(0, 0, False):
        c.wait()
    for j in range(PIECES):
        for side in range(2):
            for c in wide[side, j]:
                c.start()
    for c in copies(1, 1, False):
        c.start()
    for c in down:
        c.wait()
    diagonal_step(0, arrived)
    for c in copies(1, 1, False):
        c.wait()
    for c in copies(0, 0, True):
        c.wait()
    for c in copies(2, 0, False):
        c.start()
    diagonal_step(1, lambda side, j: None)

    def step(p, carry):
        slot = p % 2
        for c in copies(p, slot, False):
            c.wait()

        @pl.when(p < STEPS - 1)
        def _():
            for c in copies(p + 1, 1 - slot, False):
                c.start()

        @pl.when(p >= 3)
        def _():
            for c in copies(p - 2, slot, True):
                c.wait()

        for n in range(FL // 256):
            hidden_grads(slot, n)
        for c in copies(p, slot, True):
            c.start()

        @pl.when(jnp.logical_and(p >= 3, p < 7))
        def _():
            send_middle(p - 1)

        @pl.when(p == 7)
        def _():
            keep_own(6)

        for j in range(PIECES):
            for_sibling(p, slot, j)
        for j in range(PIECES):
            acc[j] = term(slot, own_col, j)
        return carry

    lax.fori_loop(2, STEPS, step, 0)
    keep_own(STEPS - 1)

    for q in range(4):
        for j in range(PIECES):
            to_first(4 + q, j).wait_recv()
            to_second(q, j).wait_recv()
            done[q, j] = (sum_own[q, j] + one_in[4 + q, j].astype(F32) + two_in[q, j].astype(F32)).astype(BF16)
            pltpu.make_async_copy(
                done.at[q, j], shard.at[pl.ds(q * U, U), pl.ds(j * W, W)], done_sem
            ).start()
    for p in (STEPS - 2, STEPS - 1):
        for c in copies(p, p % 2, True):
            c.wait()
    remote(sib_out, sib_in, sib_s, sib_r.at[0, 0], sibling).wait_send()
    remote(one_out, one_in, one_s, one_r.at[0, 0], first).wait_send()
    remote(two_out, two_in, two_s, two_r.at[0, 0], second).wait_send()
    pltpu.make_async_copy(shard, shard, done_sem).wait()


def scatter(dy, gate, up, w_gate, w_up, w_down):
    dma = pltpu.SemaphoreType.DMA
    hid = jax.ShapeDtypeStruct((ROWS, FL), BF16)
    units = lambda n: pltpu.VMEM((n, PIECES, U, W), BF16)
    steps = pltpu.VMEM((STEPS, PIECES, 2, U, W), BF16)
    return pl.pallas_call(
        scatter_kernel,
        out_shape=(jax.ShapeDtypeStruct((2 * M, HALF), BF16), hid, hid, hid),
        in_specs=[ANY] * 6,
        out_specs=(ANY,) * 4,
        scratch_shapes=[
            pltpu.VMEM((D, FL), BF16), pltpu.VMEM((D, FL), BF16), pltpu.VMEM((FL, D), BF16),
            pltpu.VMEM((2, M, D), BF16), pltpu.VMEM((2, M, FL), BF16), pltpu.VMEM((2, M, FL), BF16),
            pltpu.VMEM((2, M, FL), BF16), pltpu.VMEM((2, M, FL), BF16), pltpu.VMEM((2, M, FL), BF16),
            pltpu.VMEM((PIECES, 2, U, W), F32), pltpu.VMEM((4, PIECES, U, W), F32), units(4),
            steps, steps, units(8), units(8), units(4), units(4),
            dma((FL // 256,)), dma((2, PIECES, 2)), dma((2, 2, 3)), dma((2, 2, 3)), dma,
            dma, dma((STEPS, PIECES)), dma, dma((8, PIECES)), dma, dma((4, PIECES)),
        ],
        compiler_params=pltpu.CompilerParams(
            collective_id=0, has_side_effects=True, vmem_limit_bytes=63 * 1024 * 1024
        ),
        cost_estimate=pl.CostEstimate(
            flops=6 * ROWS * D * FL, bytes_accessed=60 * 2**20, transcendentals=2 * ROWS * FL
        ),
        name="scatter",
    )(dy, gate, up, w_gate, w_up, w_down)


def turned(a, b):
    return lax.dot_general(a, b, (((0,), (0,)), ((), ())), preferred_element_type=F32)


def wide_kernel(x, d_gate, d_up, *refs):
    dw_gate, dw_up, xt = refs[-3:]
    xt[...] = x[...].T
    dw_gate[...] = jnp.dot(xt[...], d_gate[...], preferred_element_type=F32).astype(BF16)
    dw_up[...] = jnp.dot(xt[...], d_up[...], preferred_element_type=F32).astype(BF16)


def wide_grads(x, d_gate, d_up, start, count, into=(), bm=512):
    whole = pl.BlockSpec((ROWS, FL), lambda i: (0, 0), pipeline_mode=pl.Buffered(1))
    out = pl.BlockSpec((bm, FL), lambda i: (start + i, 0))
    shape = jax.ShapeDtypeStruct((D, FL), BF16)
    return pl.pallas_call(
        wide_kernel,
        grid=(count,),
        out_shape=(shape, shape),
        in_specs=[pl.BlockSpec((ROWS, bm), lambda i: (0, start + i)), whole, whole] + [ANY] * len(into),
        out_specs=(out, out),
        scratch_shapes=[pltpu.VMEM((bm, ROWS), BF16)],
        input_output_aliases={3 + k: k for k in range(len(into))},
        compiler_params=pltpu.CompilerParams(vmem_limit_bytes=36 * 1024 * 1024),
        cost_estimate=pl.CostEstimate(flops=4 * ROWS * bm * count * FL, bytes_accessed=20 * 2**20, transcendentals=0),
        name="wide_grads",
    )(x, d_gate, d_up, *into)


def down_kernel(hidden, dy, out):
    out[...] = turned(hidden[...], dy[...]).astype(BF16)


def down_grad(hidden, dy, bn=512):
    return pl.pallas_call(
        down_kernel,
        grid=(D // bn,),
        out_shape=jax.ShapeDtypeStruct((FL, D), BF16),
        in_specs=[
            pl.BlockSpec((ROWS, FL), lambda i: (0, 0), pipeline_mode=pl.Buffered(1)),
            pl.BlockSpec((ROWS, bn), lambda i: (0, i)),
        ],
        out_specs=pl.BlockSpec((FL, bn), lambda i: (0, i)),
        compiler_params=pltpu.CompilerParams(vmem_limit_bytes=40 * 1024 * 1024),
        cost_estimate=pl.CostEstimate(flops=2 * ROWS * D * FL, bytes_accessed=24 * 2**20, transcendentals=0),
        name="down_grad",
    )(hidden, dy)


def write_kernel(spots, *refs):
    parts, out, sem = refs[: len(spots)], refs[-2], refs[-1]
    _, core, y, x = place()
    writes = []
    for k, (twin, along_first, along_second, row, count) in enumerate(spots):
        half = core + twin - 2 * core * twin
        flip_y = along_first * (1 - half) + along_second * half
        flip_x = along_first * half + along_second * (1 - half)
        to_x, to_y = x + flip_x - 2 * x * flip_x, y + flip_y - 2 * y * flip_y
        cols = pl.ds(pl.multiple_of(half * HALF, HALF), HALF)
        for i in range(0, count, U):
            rows = pl.ds(pl.multiple_of((to_x * 2 + to_y) * 2 * M + row + i, U), U)
            writes.append(pltpu.make_async_copy(parts[k].at[pl.ds(i, U)], out.at[rows, cols], sem.at[k, i // U]))
            writes[-1].start()
    for c in writes:
        c.wait()


def write(parts, spots, into=None):
    n = len(parts)
    given = () if into is None else (into,)
    return pl.pallas_call(
        functools.partial(write_kernel, spots),
        out_shape=jax.ShapeDtypeStruct((ROWS, D), BF16),
        in_specs=[pl.BlockSpec(memory_space=pltpu.VMEM)] * n + [ANY] * len(given),
        out_specs=ANY,
        scratch_shapes=[pltpu.SemaphoreType.DMA((n, 2 * M // U))],
        input_output_aliases={n: 0} if given else {},
        compiler_params=pltpu.CompilerParams(vmem_limit_bytes=16 * 1024 * 1024),
        cost_estimate=pl.CostEstimate(flops=10**9, bytes_accessed=24 * 2**20, transcendentals=0),
        name="write",
    )(*parts, *given)


def index(x, y, core):
    return (x * 2 + y) * 2 + core


def pairs(to):
    return [(index(x, y, c), index(*to(x, y, c))) for x in (0, 1) for y in (0, 1) for c in (0, 1)]


FIRST = pairs(lambda x, y, c: (x, 1 - y, c) if c == 0 else (1 - x, y, c))
SECOND = pairs(lambda x, y, c: (1 - x, y, c) if c == 0 else (x, 1 - y, c))
SIBLING = pairs(lambda x, y, c: (x, y, 1 - c))


def solution(mesh):
    def send(value, perm):
        return lax.ppermute(value, "tp", perm)

    def step(x, dy, gate, up, w_gate, w_up, w_down):
        shard, d_gate, d_up, hidden = scatter(dy, gate, up, w_gate, w_up, w_down)
        from_first, from_second = send(shard, FIRST), send(shard, SECOND)
        own_twin = send(shard, SIBLING)
        both_a = send(from_first[:M], SECOND)
        both_b = send(from_first[M:], SECOND)
        first_twin = send(from_first, SIBLING)
        second_twin = send(from_second, SIBLING)
        twin_a, twin_b = send(both_a, SIBLING), send(both_b, SIBLING)
        dw_down = down_grad(hidden, dy)
        wide = wide_grads(x, d_gate, d_up, 0, 3)
        dw_gate, dw_up = wide_grads(x, d_gate, d_up, 3, 3, wide)
        dx = write(
            (shard, own_twin, from_first, first_twin, from_second, second_twin),
            tuple((t, f, s, 0, 2 * M) for f, s in ((0, 0), (1, 0), (0, 1)) for t in (0, 1)),
        )
        dx = write(
            (both_a, both_b, twin_a, twin_b),
            tuple((t, 1, 1, r, M) for t in (0, 1) for r in (0, M)),
            dx,
        )
        return dx, dw_gate, dw_up, dw_down

    tokens, columns, rows = P("dp", None), P(None, "tp"), P("tp", None)
    return jax.shard_map(
        step,
        mesh=mesh,
        in_specs=(tokens, tokens, P("dp", "tp"), P("dp", "tp"), columns, columns, rows),
        out_specs=(tokens, P("dp", "tp"), P("dp", "tp"), P(("dp", "tp"), None)),
        check_vma=False,
    )
```

```python
import functools

import jax
import jax.numpy as jnp
from jax import lax
from jax.experimental import pallas as pl
from jax.experimental.pallas import tpu as pltpu
from jax.sharding import PartitionSpec as P


SCATTER_MIB, WIDE_MIB, DOWN_MIB = 47, 26, 26

BF16, F32 = jnp.bfloat16, jnp.float32
ROWS, D, FL = 2048, 3072, 1024
M = 256
U = M // 2
HALF = D // 2
W = 512
PIECES = HALF // W
BN = 512
PARTS = D // BN
STEPS = ROWS // M
ANY = pl.BlockSpec(memory_space=pl.ANY)


def nt(a, b):
    return lax.dot_general(a, b, (((1,), (1,)), ((), ())), preferred_element_type=F32)


def turned(a, b):
    return lax.dot_general(a, b, (((0,), (0,)), ((), ())), preferred_element_type=F32)


def places(parts, spots, out, sem):
    _, core, y, x = place()
    copies = []
    for k, (part, (twin, along_first, along_second, row, count)) in enumerate(zip(parts, spots)):
        half = core + twin - 2 * core * twin
        flip_y = along_first * (1 - half) + along_second * half
        flip_x = along_first * half + along_second * (1 - half)
        to_x, to_y = x + flip_x - 2 * x * flip_x, y + flip_y - 2 * y * flip_y
        cols = pl.ds(pl.multiple_of(half * HALF, HALF), HALF)
        for i in range(0, count, U):
            rows = pl.ds(pl.multiple_of((to_x * 2 + to_y) * 2 * M + row + i, U), U)
            copies.append(pltpu.make_async_copy(part.at[pl.ds(i, U)], out.at[rows, cols], sem.at[k, i // U]))
    return copies


def place():
    me = lax.axis_index("tp")
    core, y, x = me % 2, (me // 2) % 2, me // 4
    return me, core, y, x


def rows_of(p, x, y):
    diag, own = 1 - jnp.minimum(p // 2, 1), p // 6
    mid = 1 - diag - own
    at = diag * p * M + own * (p - 6) * M + mid * (p - 2) * U

    def run(flip_x, flip_y):
        to_x, to_y = x + flip_x - 2 * x * flip_x, y + flip_y - 2 * y * flip_y
        return (to_x * 2 + to_y) * 2 * M + at

    return run(diag, diag + mid), run(diag + mid, diag) + (1 - mid) * U


def scatter_kernel(
    dy, gate, up, w_gate, w_up, w_down,
    shard, d_gate, d_up, hidden, block,
    wg, wu, wd, dyb, gb, ub, dgb, dub, acc, sum_own,
    sib_out, sib_in, one_out, one_in, two_out, two_in,
    down_sem, wide_sem, in_sem,
    sib_s, sib_r, one_s, one_r, two_s, two_r,
):
    me, core, y, x = place()
    sibling = me + 1 - 2 * core
    near_x, near_y = me + 4 - 8 * x, me + 2 - 4 * y
    first = near_y * (1 - core) + near_x * core
    second = near_x * (1 - core) + near_y * core
    own_col, sib_col = core * HALF, (1 - core) * HALF

    def inputs(p, slot):
        made = []
        for h, row in enumerate(rows_of(p, x, y)):
            rows = pl.ds(pl.multiple_of(row, U), U)
            for k, (near, far) in enumerate(((dyb, dy), (gb, gate), (ub, up))):
                made.append(pltpu.make_async_copy(far.at[rows], near.at[slot, pl.ds(h * U, U)], in_sem.at[slot, h, k]))
        return made

    def columns(base, j):
        return pl.ds(pl.multiple_of(base + j * W, 256), W)

    down = []
    for n in range(FL // 256):
        at = pl.ds(n * 256, 256)
        down.append(pltpu.make_async_copy(w_down.at[at], wd.at[at], down_sem.at[n]))
    wide = {}
    for j in range(PIECES):
        for side, base in ((0, sib_col), (1, own_col)):
            at = columns(base, j)
            wide[side, j] = (
                pltpu.make_async_copy(w_gate.at[at], wg.at[at], wide_sem.at[side, j, 0]),
                pltpu.make_async_copy(w_up.at[at], wu.at[at], wide_sem.at[side, j, 1]),
            )

    def remote(src, dst, send, recv, to):
        return pltpu.make_async_remote_copy(
            src_ref=src, dst_ref=dst, send_sem=send, recv_sem=recv,
            device_id={"tp": to}, device_id_type=pl.DeviceIdType.MESH,
        )

    def to_sibling(p, j):
        return remote(sib_out.at[p % 2, j], sib_in.at[p % 2, j], sib_s.at[p % 2, j], sib_r.at[p % 2, j], sibling)

    def to_first(k, j):
        return remote(one_out.at[k, j], one_in.at[k, j], one_s, one_r.at[k, j], first)

    def to_second(k, j):
        return remote(two_out.at[k, j], two_in.at[k, j], two_s, two_r.at[k, j], second)

    for c in inputs(0, 0):
        c.start()
    for c in down:
        c.start()

    barrier = pltpu.get_barrier_semaphore()
    for other in (sibling, first, second):
        pl.semaphore_signal(barrier, inc=1, device_id={"tp": other}, device_id_type=pl.DeviceIdType.MESH)
    pl.semaphore_wait(barrier, 3)

    def keep(to, p, at, value):
        value = value.astype(BF16)
        for h, row in enumerate(rows_of(p, x, y)):
            to[pl.ds(pl.multiple_of(row, U), U), at] = value[h * U : (h + 1) * U]
        return value

    def hidden_grads(p, slot, n):
        at = slice(n * 256, (n + 1) * 256)
        d_hidden = nt(dyb[slot], wd[at, :])
        g, u = gb[slot, :, at].astype(F32), ub[slot, :, at].astype(F32)
        s = jax.nn.sigmoid(g)
        act = g * s
        keep(hidden, p, at, act * u)
        dub[:, at] = keep(d_up, p, at, d_hidden * act)
        dgb[:, at] = keep(d_gate, p, at, d_hidden * u * (s + act * (1 - s)))

    def term(base, j):
        at = columns(base, j)
        return (nt(dgb[...], wg[at, :]) + nt(dub[...], wu[at, :])).reshape(2, U, W)

    def for_sibling(p, j, reused):
        if reused:
            to_sibling(p, j).wait_send()
        sib_out[p % 2, j] = term(sib_col, j).astype(BF16)
        to_sibling(p, j).start()

    def chip_sum(p, j, h):
        return acc[j, h] + sib_in[p % 2, j, h].astype(F32)

    def send_diagonal(p, j):
        for h in range(2):
            one_out[2 * p + h, j] = chip_sum(p, j, h).astype(BF16)
            to_first(2 * p + h, j).start()

    def send_middle(p):
        q = p - 2
        for j in range(PIECES):
            to_sibling(p, j).wait_recv()
            one_out[4 + q, j] = chip_sum(p, j, core).astype(BF16)
            to_first(4 + q, j).start()
        for j in range(PIECES):
            to_first(q, j).wait_recv()
            two_out[q, j] = (chip_sum(p, j, 1 - core) + one_in[q, j].astype(F32)).astype(BF16)
            to_second(q, j).start()

    def keep_own(p):
        for j in range(PIECES):
            to_sibling(p, j).wait_recv()
            for h in range(2):
                sum_own[2 * (p - 6) + h, j] = chip_sum(p, j, h)

    def diagonal_step(p, ready):
        for n in range(FL // 256):
            hidden_grads(p, p, n)
        for j in range(PIECES + 1):
            if j < PIECES:
                ready(0, j)
                for_sibling(p, j, False)
            if j:
                ready(1, j - 1)
                acc[j - 1] = term(own_col, j - 1)
                to_sibling(p, j - 1).wait_recv()
                send_diagonal(p, j - 1)

    def arrived(side, j):
        for c in wide[side, j]:
            c.wait()

    down_inputs = []
    for k in range(ROWS // M):
        near = dyb.at[k // PARTS, :, pl.ds(k % PARTS * BN, BN)]
        down_inputs.append(
            pltpu.make_async_copy(dy.at[pl.ds(k * M, M), pl.ds(0, BN)], near, in_sem.at[k // 6, k % 6 // 3, k % 3])
        )

    for c in inputs(0, 0):
        c.wait()
    for j in range(PIECES):
        for side in range(2):
            for c in wide[side, j]:
                c.start()
    for c in inputs(1, 1):
        c.start()
    for c in down:
        c.wait()
    diagonal_step(0, arrived)
    for c in inputs(1, 1):
        c.wait()
    for c in inputs(2, 0):
        c.start()
    diagonal_step(1, lambda side, j: None)

    def step(p, carry):
        slot = p % 2
        for c in inputs(p, slot):
            c.wait()

        @pl.when(p < STEPS - 1)
        def _():
            for c in inputs(p + 1, 1 - slot):
                c.start()

        for n in range(FL // 256):
            hidden_grads(p, slot, n)

        @pl.when(jnp.logical_and(p >= 4, p < 7))
        def _():
            send_middle(p - 1)

        @pl.when(p == 7)
        def _():
            for c in down_inputs:
                c.start()
            keep_own(6)

        for j in range(PIECES):
            for_sibling(p, j, True)
        for j in range(PIECES):
            acc[j] = term(own_col, j)

        @pl.when(p == 2)
        def _():
            send_middle(2)

        return carry

    lax.fori_loop(2, STEPS, step, 0)
    keep_own(STEPS - 1)

    for c in down_inputs:
        c.wait()
    for n in range(0, BN, 256):
        right = jnp.concatenate([dyb[k // PARTS, :, pl.ds(k % PARTS * BN + n, 256)] for k in range(ROWS // M)])
        block[:, pl.ds(n, 256)] = turned(hidden[...], right).astype(BF16)

    for q in range(4):
        for j in range(PIECES):
            to_first(4 + q, j).wait_recv()
            to_second(q, j).wait_recv()
            total = sum_own[q, j] + one_in[4 + q, j].astype(F32) + two_in[q, j].astype(F32)
            shard[pl.ds(q * U, U), pl.ds(j * W, W)] = total.astype(BF16)
    for p in (STEPS - 2, STEPS - 1):
        for j in range(PIECES):
            to_sibling(p, j).wait_send()
    remote(one_out, one_in, one_s, one_r.at[0, 0], first).wait_send()
    remote(two_out, two_in, two_s, two_r.at[0, 0], second).wait_send()


def scatter(dy, gate, up, w_gate, w_up, w_down):
    dma = pltpu.SemaphoreType.DMA
    hid = pltpu.VMEM((ROWS, FL), BF16)
    units = lambda n: pltpu.VMEM((n, PIECES, U, W), BF16)
    twin = pltpu.VMEM((2, PIECES, 2, U, W), BF16)
    return pl.pallas_call(
        scatter_kernel,
        out_shape=(pltpu.VMEM((2 * M, HALF), BF16), hid, hid, hid, pltpu.VMEM((FL, BN), BF16)),
        in_specs=[ANY] * 6,
        out_specs=(pl.BlockSpec(memory_space=pltpu.VMEM),) * 5,
        scratch_shapes=[
            pltpu.VMEM((D, FL), BF16), pltpu.VMEM((D, FL), BF16), pltpu.VMEM((FL, D), BF16),
            pltpu.VMEM((2, M, D), BF16), pltpu.VMEM((2, M, FL), BF16), pltpu.VMEM((2, M, FL), BF16),
            pltpu.VMEM((M, FL), BF16), pltpu.VMEM((M, FL), BF16),
            pltpu.VMEM((PIECES, 2, U, W), F32), pltpu.VMEM((4, PIECES, U, W), F32),
            twin, twin, units(8), units(8), units(4), units(4),
            dma((FL // 256,)), dma((2, PIECES, 2)), dma((2, 2, 3)),
            dma((2, PIECES)), dma((2, PIECES)), dma, dma((8, PIECES)), dma, dma((4, PIECES)),
        ],
        compiler_params=pltpu.CompilerParams(
            collective_id=0, has_side_effects=True, vmem_limit_bytes=SCATTER_MIB * 2**20
        ),
        cost_estimate=pl.CostEstimate(
            flops=6 * ROWS * D * FL, bytes_accessed=60 * 2**20, transcendentals=2 * ROWS * FL
        ),
        name="scatter",
    )(dy, gate, up, w_gate, w_up, w_down)


def placed(value, space):
    return pltpu.with_memory_space_constraint(value, space)


def wide_kernel(x, d_gate, d_up, *refs):
    dw_gate, dw_up = refs[-2:]
    xt = x[...].T
    dw_gate[...] = jnp.dot(xt, d_gate[...], preferred_element_type=F32).astype(BF16)
    dw_up[...] = jnp.dot(xt, d_up[...], preferred_element_type=F32).astype(BF16)


def wide_grads(x, d_gate, d_up, start, count, into=(), bm=512):
    whole = pl.BlockSpec((ROWS, FL), lambda i: (0, 0), pipeline_mode=pl.Buffered(1))
    out = pl.BlockSpec((bm, FL), lambda i: (start + i, 0))
    shape = jax.ShapeDtypeStruct((D, FL), BF16)
    return pl.pallas_call(
        wide_kernel,
        grid=(count,),
        out_shape=(shape, shape),
        in_specs=[pl.BlockSpec((ROWS, bm), lambda i: (0, start + i)), whole, whole] + [ANY] * len(into),
        out_specs=(out, out),
        input_output_aliases={3 + k: k for k in range(len(into))},
        compiler_params=pltpu.CompilerParams(vmem_limit_bytes=WIDE_MIB * 2**20),
        cost_estimate=pl.CostEstimate(flops=4 * ROWS * bm * count * FL, bytes_accessed=20 * 2**20, transcendentals=0),
        name="wide_grads",
    )(placed(x, pltpu.HBM), placed(d_gate, pltpu.VMEM), placed(d_up, pltpu.VMEM), *into)


def down_kernel(spots, hidden, dy, block, *refs):
    n = len(spots)
    parts, out, dx, sem = refs[:n], refs[n], refs[n + 1], refs[n + 2]
    step, last = pl.program_id(0), pl.num_programs(0) - 1

    @pl.when(step == 0)
    def _():
        for c in places(parts, spots, dx, sem):
            c.start()

    @pl.when(step < last)
    def _():
        out[...] = turned(hidden[...], dy[...]).astype(BF16)

    @pl.when(step == last)
    def _():
        out[...] = block[...]
        for c in places(parts, spots, dx, sem):
            c.wait()


def down_grad(hidden, dy, block, parts, spots):
    n = len(parts)
    whole = lambda *shape: pl.BlockSpec(shape, lambda i: (0, 0), pipeline_mode=pl.Buffered(1))
    return pl.pallas_call(
        functools.partial(down_kernel, spots),
        grid=(PARTS,),
        out_shape=(jax.ShapeDtypeStruct((FL, D), BF16), jax.ShapeDtypeStruct((ROWS, D), BF16)),
        in_specs=[
            whole(ROWS, FL), pl.BlockSpec((ROWS, BN), lambda i: (0, jnp.minimum(i + 1, PARTS - 1))), whole(FL, BN),
        ]
        + [ANY] * n,
        out_specs=(pl.BlockSpec((FL, BN), lambda i: (0, (i + 1) % PARTS)), ANY),
        scratch_shapes=[pltpu.SemaphoreType.DMA((n, 2 * M // U))],
        compiler_params=pltpu.CompilerParams(vmem_limit_bytes=DOWN_MIB * 2**20),
        cost_estimate=pl.CostEstimate(flops=2 * ROWS * D * FL, bytes_accessed=24 * 2**20, transcendentals=0),
        name="down_grad",
    )(placed(hidden, pltpu.VMEM), placed(dy, pltpu.HBM), placed(block, pltpu.VMEM), *parts)


def write_kernel(spots, *refs):
    copies = places(refs[: len(spots)], spots, refs[-2], refs[-1])
    for c in copies:
        c.start()
    for c in copies:
        c.wait()


def write(parts, spots, into=None):
    n = len(parts)
    given = () if into is None else (into,)
    return pl.pallas_call(
        functools.partial(write_kernel, spots),
        out_shape=jax.ShapeDtypeStruct((ROWS, D), BF16),
        in_specs=[pl.BlockSpec(memory_space=pltpu.VMEM)] * n + [ANY] * len(given),
        out_specs=ANY,
        scratch_shapes=[pltpu.SemaphoreType.DMA((n, 2 * M // U))],
        input_output_aliases={n: 0} if given else {},
        compiler_params=pltpu.CompilerParams(vmem_limit_bytes=16 * 1024 * 1024),
        cost_estimate=pl.CostEstimate(flops=10**9, bytes_accessed=24 * 2**20, transcendentals=0),
        name="write",
    )(*parts, *given)


def index(x, y, core):
    return (x * 2 + y) * 2 + core


def pairs(to):
    return [(index(x, y, c), index(*to(x, y, c))) for x in (0, 1) for y in (0, 1) for c in (0, 1)]


FIRST = pairs(lambda x, y, c: (x, 1 - y, c) if c == 0 else (1 - x, y, c))
SECOND = pairs(lambda x, y, c: (1 - x, y, c) if c == 0 else (x, 1 - y, c))
SIBLING = pairs(lambda x, y, c: (x, y, 1 - c))


def solution(mesh):
    def send(value, perm):
        return lax.ppermute(value, "tp", perm)

    def step(x, dy, gate, up, w_gate, w_up, w_down):
        shard, d_gate, d_up, hidden, block = scatter(dy, gate, up, w_gate, w_up, w_down)
        first_a, first_b = send(shard[:M], FIRST), send(shard[M:], FIRST)
        second = send(shard, SECOND)
        own_twin = send(shard, SIBLING)
        both_a, both_b = send(first_a, SECOND), send(first_b, SECOND)
        first_a_twin, first_b_twin = send(first_a, SIBLING), send(first_b, SIBLING)
        second_twin = send(second, SIBLING)
        both_a_twin, both_b_twin = send(both_a, SIBLING), send(both_b, SIBLING)
        wide = wide_grads(x, d_gate, d_up, 0, 3)
        dw_gate, dw_up = wide_grads(x, d_gate, d_up, 3, 3, wide)
        dw_down, dx = down_grad(
            hidden, dy, block, (shard, own_twin, first_a, first_a_twin, first_b, second),
            ((0, 0, 0, 0, 2 * M), (1, 0, 0, 0, 2 * M), (0, 1, 0, 0, M), (1, 1, 0, 0, M), (0, 1, 0, M, M), (0, 0, 1, 0, 2 * M)),
        )
        dx = write(
            (first_b_twin, second_twin, both_a, both_b),
            ((1, 1, 0, M, M), (1, 0, 1, 0, 2 * M), (0, 1, 1, 0, M), (0, 1, 1, M, M)),
            dx,
        )
        dx = write((both_a_twin, both_b_twin), ((1, 1, 1, 0, M), (1, 1, 1, M, M)), dx)
        return dx, dw_gate, dw_up, dw_down

    tokens, columns, rows = P("dp", None), P(None, "tp"), P("tp", None)
    return jax.shard_map(
        step,
        mesh=mesh,
        in_specs=(tokens, tokens, P("dp", "tp"), P("dp", "tp"), columns, columns, rows),
        out_specs=(tokens, P("dp", "tp"), P("dp", "tp"), P(("dp", "tp"), None)),
        check_vma=False,
    )
```

```python
import functools

import jax
import jax.numpy as jnp
from jax import lax
from jax.experimental import pallas as pl
from jax.experimental.pallas import tpu as pltpu
from jax.sharding import PartitionSpec as P


SCATTER_MIB, WIDE_MIB, DOWN_MIB = 44, 26, 26

BF16, F32 = jnp.bfloat16, jnp.float32
ROWS, D, FL = 2048, 3072, 1024
M = 256
U = M // 2
HALF = D // 2
W = 512
PIECES = HALF // W
BN = 512
EARLY = 3 * BN
LATE = (D - EARLY) // BN
STEPS = ROWS // M
ANY = pl.BlockSpec(memory_space=pl.ANY)


def nt(a, b):
    return lax.dot_general(a, b, (((1,), (1,)), ((), ())), preferred_element_type=F32)


def turned(a, b):
    return lax.dot_general(a, b, (((0,), (0,)), ((), ())), preferred_element_type=F32)


def places(parts, spots, out, sem):
    _, core, y, x = place()
    copies = []
    for k, (part, (twin, along_first, along_second, row, count)) in enumerate(zip(parts, spots)):
        half = core + twin - 2 * core * twin
        flip_y = along_first * (1 - half) + along_second * half
        flip_x = along_first * half + along_second * (1 - half)
        to_x, to_y = x + flip_x - 2 * x * flip_x, y + flip_y - 2 * y * flip_y
        cols = pl.ds(pl.multiple_of(half * HALF, HALF), HALF)
        for i in range(0, count, U):
            rows = pl.ds(pl.multiple_of((to_x * 2 + to_y) * 2 * M + row + i, U), U)
            copies.append(pltpu.make_async_copy(part.at[pl.ds(i, U)], out.at[rows, cols], sem.at[k, i // U]))
    return copies


def place():
    me = lax.axis_index("tp")
    core, y, x = me % 2, (me // 2) % 2, me // 4
    return me, core, y, x


def rows_of(p, x, y):
    diag, own = 1 - jnp.minimum(p // 2, 1), p // 6
    mid = 1 - diag - own
    at = diag * p * M + own * (p - 6) * M + mid * (p - 2) * U

    def run(flip_x, flip_y):
        to_x, to_y = x + flip_x - 2 * x * flip_x, y + flip_y - 2 * y * flip_y
        return (to_x * 2 + to_y) * 2 * M + at

    return run(diag, diag + mid), run(diag + mid, diag) + (1 - mid) * U


def scatter_kernel(
    dy, gate, up, w_gate, w_up, w_down,
    shard, upper, lower, d_gate, d_up, hidden, block,
    wide, wd, inb, dgb, dub, acc, sum_own,
    sib_out, sib_in, one_out, one_in, two_out, two_in,
    down_sem, wide_sem, in_sem,
    sib_s, sib_r, one_s, one_r, two_s, two_r,
):
    me, core, y, x = place()
    sibling = me + 1 - 2 * core
    near_x, near_y = me + 4 - 8 * x, me + 2 - 4 * y
    first = near_y * (1 - core) + near_x * core
    second = near_x * (1 - core) + near_y * core
    own_col, sib_col = core * HALF, (1 - core) * HALF

    def inputs(p, slot):
        made = []
        for h, row in enumerate(rows_of(p, x, y)):
            rows, at = pl.ds(pl.multiple_of(row, U), U), 0
            for far in (dy, gate, up):
                near = inb.at[slot, pl.ds(h * U, U), pl.ds(at, far.shape[1])]
                made.append(pltpu.make_async_copy(far.at[rows], near, in_sem.at[slot]))
                at += far.shape[1]
        return made

    def inputs_here(slot):
        pltpu.make_async_copy(inb.at[slot], inb.at[slot], in_sem.at[slot]).wait()

    def columns(base, j):
        return pl.ds(pl.multiple_of(base + j * W, 256), W)

    down = []
    for n in range(FL // 256):
        at = pl.ds(n * 256, 256)
        down.append(pltpu.make_async_copy(w_down.at[at], wd.at[at], down_sem.at[n]))
    slices = {}
    for j in range(PIECES):
        for side, base in ((0, sib_col), (1, own_col)):
            at = columns(base, j)
            slices[side, j] = [
                pltpu.make_async_copy(w.at[at], wide.at[k, at], wide_sem.at[side, j])
                for k, w in enumerate((w_gate, w_up))
            ]

    def remote(src, dst, send, recv, to):
        return pltpu.make_async_remote_copy(
            src_ref=src, dst_ref=dst, send_sem=send, recv_sem=recv,
            device_id={"tp": to}, device_id_type=pl.DeviceIdType.MESH,
        )

    def to_sibling(p, j):
        return remote(sib_out.at[p % 2, j], sib_in.at[p % 2, j], sib_s.at[p % 2, j], sib_r.at[p % 2, j], sibling)

    def to_first(k, j):
        return remote(one_out.at[k, j], one_in.at[k, j], one_s, one_r.at[k, j], first)

    def to_second(k, j):
        return remote(two_out.at[k, j], two_in.at[k, j], two_s, two_r.at[k, j], second)

    for c in inputs(0, 0) + down[:2]:
        c.start()

    barrier = pltpu.get_barrier_semaphore()
    for other in (sibling, first, second):
        pl.semaphore_signal(barrier, inc=1, device_id={"tp": other}, device_id_type=pl.DeviceIdType.MESH)
    pl.semaphore_wait(barrier, 3)
    for c in down[2:]:
        c.start()

    def keep(to, p, at, value):
        value = value.astype(BF16)
        for h, row in enumerate(rows_of(p, x, y)):
            to[pl.ds(pl.multiple_of(row, U), U), at] = value[h * U : (h + 1) * U]
        return value

    def hidden_grads(p, slot, n):
        at = slice(n * 256, (n + 1) * 256)
        d_hidden = nt(inb[slot, :, :D], wd[at, :])
        g = inb[slot, :, D + n * 256 : D + (n + 1) * 256].astype(F32)
        u = inb[slot, :, D + FL + n * 256 : D + FL + (n + 1) * 256].astype(F32)
        s = jax.nn.sigmoid(g)
        act = g * s
        keep(hidden, p, at, act * u)
        dub[:, at] = keep(d_up, p, at, d_hidden * act)
        dgb[:, at] = keep(d_gate, p, at, d_hidden * u * (s + act * (1 - s)))

    def term(base, j):
        at = columns(base, j)
        return (nt(dgb[...], wide[0, at, :]) + nt(dub[...], wide[1, at, :])).reshape(2, U, W)

    def for_sibling(p, pieces):
        for j in pieces:
            sib_out[p % 2, j] = term(sib_col, j).astype(BF16)
        for j in pieces:
            to_sibling(p, j).start()

    def chip_sum(p, j, h):
        return acc[j, h] + sib_in[p % 2, j, h].astype(F32)

    def send_diagonal(p, j):
        for h in range(2):
            one_out[2 * p + h, j] = chip_sum(p, j, h).astype(BF16)
            to_first(2 * p + h, j).start()

    def send_middle(p):
        q = p - 2
        for j in range(PIECES):
            to_sibling(p, j).wait_recv()
            one_out[4 + q, j] = chip_sum(p, j, core).astype(BF16)
            to_first(4 + q, j).start()
        for j in range(PIECES):
            to_first(q, j).wait_recv()
            two_out[q, j] = (chip_sum(p, j, 1 - core) + one_in[q, j].astype(F32)).astype(BF16)
            to_second(q, j).start()

    def keep_own(p):
        for j in range(PIECES):
            to_sibling(p, j).wait_recv()
            for h in range(2):
                sum_own[2 * (p - 6) + h, j] = chip_sum(p, j, h)

    def diagonal_step(p, ready):
        for j in range(PIECES + 1):
            if j < PIECES:
                ready(0, j)
                for_sibling(p, (j,))
            if j:
                ready(1, j - 1)
                acc[j - 1] = term(own_col, j - 1)
                to_sibling(p, j - 1).wait_recv()
                send_diagonal(p, j - 1)

    def arrived(side, j):
        here = wide.at[:, columns((sib_col, own_col)[side], j)]
        pltpu.make_async_copy(here, here, wide_sem.at[side, j]).wait()

    down_inputs = []
    for k in range(ROWS // FL):
        near = wd.at[:, pl.ds(k * EARLY, EARLY)]
        down_inputs.append(pltpu.make_async_copy(dy.at[pl.ds(k * FL, FL), pl.ds(0, EARLY)], near, down_sem.at[k]))

    inputs_here(0)
    for c in down[:2]:
        c.wait()
    for c in slices[0, 0] + slices[0, 1]:
        c.start()
    for n in range(2):
        hidden_grads(0, 0, n)
    for c in down[2:]:
        c.wait()
    for k in ((1, 0), (0, 2), (1, 1), (1, 2)):
        for c in slices[k]:
            c.start()
    for c in inputs(1, 1):
        c.start()
    for n in range(2, 4):
        hidden_grads(0, 0, n)
    diagonal_step(0, arrived)
    inputs_here(1)
    for c in inputs(2, 0):
        c.start()
    for n in range(FL // 256):
        hidden_grads(1, 1, n)
    diagonal_step(1, lambda side, j: None)

    def step(p, carry):
        slot = p % 2
        inputs_here(slot)

        @pl.when(p < STEPS - 1)
        def _():
            for c in inputs(p + 1, 1 - slot):
                c.start()

        for n in range(FL // 256):
            hidden_grads(p, slot, n)

        @pl.when(jnp.logical_and(p >= 4, p < 7))
        def _():
            send_middle(p - 1)

        @pl.when(p == 7)
        def _():
            for c in down_inputs:
                c.start()
            keep_own(6)

        for j in range(PIECES):
            to_sibling(p, j).wait_send()
        for_sibling(p, range(PIECES))
        for j in range(PIECES):
            acc[j] = term(own_col, j)

        @pl.when(p == 2)
        def _():
            send_middle(2)

        return carry

    lax.fori_loop(2, STEPS, step, 0)
    keep_own(STEPS - 1)

    for c in down_inputs:
        c.wait()
    for n in range(0, EARLY, 256):
        right = jnp.concatenate([wd[:, pl.ds(k * EARLY + n, 256)] for k in range(ROWS // FL)])
        block[:, pl.ds(n, 256)] = turned(hidden[...], right).astype(BF16)

    for q in range(4):
        for j in range(PIECES):
            to_first(4 + q, j).wait_recv()
            to_second(q, j).wait_recv()
            total = sum_own[q, j] + one_in[4 + q, j].astype(F32) + two_in[q, j].astype(F32)
            for to, row in ((upper, lower)[q // 2], q % 2), (shard, q):
                to[pl.ds(row * U, U), pl.ds(j * W, W)] = total.astype(BF16)
    for p in (STEPS - 2, STEPS - 1):
        for j in range(PIECES):
            to_sibling(p, j).wait_send()
    remote(one_out, one_in, one_s, one_r.at[0, 0], first).wait_send()
    remote(two_out, two_in, two_s, two_r.at[0, 0], second).wait_send()


def scatter(dy, gate, up, w_gate, w_up, w_down):
    dma = pltpu.SemaphoreType.DMA
    hid, part = pltpu.VMEM((ROWS, FL), BF16), pltpu.VMEM((M, HALF), BF16)
    units = lambda n: pltpu.VMEM((n, PIECES, U, W), BF16)
    twin = pltpu.VMEM((2, PIECES, 2, U, W), BF16)
    return pl.pallas_call(
        scatter_kernel,
        out_shape=(pltpu.VMEM((2 * M, HALF), BF16), part, part, hid, hid, hid, pltpu.VMEM((FL, EARLY), BF16)),
        in_specs=[ANY] * 6,
        out_specs=(pl.BlockSpec(memory_space=pltpu.VMEM),) * 7,
        scratch_shapes=[
            pltpu.VMEM((2, D, FL), BF16), pltpu.VMEM((FL, D), BF16), pltpu.VMEM((2, M, D + 2 * FL), BF16),
            pltpu.VMEM((M, FL), BF16), pltpu.VMEM((M, FL), BF16),
            pltpu.VMEM((PIECES, 2, U, W), F32), pltpu.VMEM((4, PIECES, U, W), F32),
            twin, twin, units(8), units(8), units(4), units(4),
            dma((FL // 256,)), dma((2, PIECES)), dma((2,)),
            dma((2, PIECES)), dma((2, PIECES)), dma, dma((8, PIECES)), dma, dma((4, PIECES)),
        ],
        compiler_params=pltpu.CompilerParams(
            collective_id=0, has_side_effects=True, vmem_limit_bytes=SCATTER_MIB * 2**20
        ),
        cost_estimate=pl.CostEstimate(
            flops=6 * ROWS * D * FL, bytes_accessed=60 * 2**20, transcendentals=2 * ROWS * FL
        ),
        name="scatter",
    )(dy, gate, up, w_gate, w_up, w_down)


def placed(value, space):
    return pltpu.with_memory_space_constraint(value, space)


def wide_kernel(x, d_gate, d_up, *refs):
    dw_gate, dw_up = refs[-2:]
    xt = x[...].T
    dw_gate[...] = jnp.dot(xt, d_gate[...], preferred_element_type=F32).astype(BF16)
    dw_up[...] = jnp.dot(xt, d_up[...], preferred_element_type=F32).astype(BF16)


def wide_grads(x, d_gate, d_up, start, count, into=(), bm=512):
    whole = pl.BlockSpec((ROWS, FL), lambda i: (0, 0), pipeline_mode=pl.Buffered(1))
    out = pl.BlockSpec((bm, FL), lambda i: (start + i, 0))
    shape = jax.ShapeDtypeStruct((D, FL), BF16)
    return pl.pallas_call(
        wide_kernel,
        grid=(count,),
        out_shape=(shape, shape),
        in_specs=[pl.BlockSpec((ROWS, bm), lambda i: (0, start + i)), whole, whole] + [ANY] * len(into),
        out_specs=(out, out),
        input_output_aliases={3 + k: k for k in range(len(into))},
        compiler_params=pltpu.CompilerParams(vmem_limit_bytes=WIDE_MIB * 2**20),
        cost_estimate=pl.CostEstimate(flops=4 * ROWS * bm * count * FL, bytes_accessed=20 * 2**20, transcendentals=0),
        name="wide_grads",
    )(placed(x, pltpu.HBM), placed(d_gate, pltpu.VMEM), placed(d_up, pltpu.VMEM), *into)


def down_kernel(spots, hidden, dy, block, *refs):
    n = len(spots)
    parts, (out, dx, made, part_sem, block_sem, made_sem) = refs[:n], refs[n:]
    step, last = pl.program_id(0), pl.num_programs(0) - 1

    def save(i):
        cols = pl.ds(pl.multiple_of(EARLY + i * BN, BN), BN)
        return pltpu.make_async_copy(made.at[i % 2], out.at[:, cols], made_sem.at[i % 2])

    early = pltpu.make_async_copy(block, out.at[:, pl.ds(0, EARLY)], block_sem)

    @pl.when(step == 0)
    def _():
        early.start()
        for c in places(parts, spots, dx, part_sem):
            c.start()

    @pl.when(step >= 2)
    def _():
        save(step - 2).wait()

    made[step % 2] = turned(hidden[...], dy[...]).astype(BF16)
    save(step).start()

    @pl.when(step == last)
    def _():
        early.wait()
        for c in places(parts, spots, dx, part_sem):
            c.wait()
        save(step - 1).wait()
        save(step).wait()


def down_grad(hidden, dy, block, parts, spots):
    n = len(parts)
    dma = pltpu.SemaphoreType.DMA
    whole = lambda *shape: pl.BlockSpec(shape, lambda i: (0, 0), pipeline_mode=pl.Buffered(1))
    return pl.pallas_call(
        functools.partial(down_kernel, spots),
        grid=(LATE,),
        out_shape=(jax.ShapeDtypeStruct((FL, D), BF16), jax.ShapeDtypeStruct((ROWS, D), BF16)),
        in_specs=[whole(ROWS, FL), pl.BlockSpec((ROWS, BN), lambda i: (0, i + EARLY // BN)), whole(FL, EARLY)]
        + [ANY] * n,
        out_specs=(ANY, ANY),
        scratch_shapes=[pltpu.VMEM((2, FL, BN), BF16), dma((n, 2 * M // U)), dma, dma((2,))],
        compiler_params=pltpu.CompilerParams(vmem_limit_bytes=DOWN_MIB * 2**20),
        cost_estimate=pl.CostEstimate(flops=2 * ROWS * D * FL, bytes_accessed=24 * 2**20, transcendentals=0),
        name="down_grad",
    )(placed(hidden, pltpu.VMEM), placed(dy, pltpu.HBM), placed(block, pltpu.VMEM), *parts)


def write_kernel(spots, *refs):
    copies = places(refs[: len(spots)], spots, refs[-2], refs[-1])
    for c in copies:
        c.start()
    for c in copies:
        c.wait()


def write(parts, spots, into=None):
    n = len(parts)
    given = () if into is None else (into,)
    return pl.pallas_call(
        functools.partial(write_kernel, spots),
        out_shape=jax.ShapeDtypeStruct((ROWS, D), BF16),
        in_specs=[pl.BlockSpec(memory_space=pltpu.VMEM)] * n + [ANY] * len(given),
        out_specs=ANY,
        scratch_shapes=[pltpu.SemaphoreType.DMA((n, 2 * M // U))],
        input_output_aliases={n: 0} if given else {},
        compiler_params=pltpu.CompilerParams(vmem_limit_bytes=16 * 1024 * 1024),
        cost_estimate=pl.CostEstimate(flops=10**9, bytes_accessed=24 * 2**20, transcendentals=0),
        name="write",
    )(*parts, *given)


def index(x, y, core):
    return (x * 2 + y) * 2 + core


def pairs(to):
    return [(index(x, y, c), index(*to(x, y, c))) for x in (0, 1) for y in (0, 1) for c in (0, 1)]


FIRST = pairs(lambda x, y, c: (x, 1 - y, c) if c == 0 else (1 - x, y, c))
SECOND = pairs(lambda x, y, c: (1 - x, y, c) if c == 0 else (x, 1 - y, c))
SIBLING = pairs(lambda x, y, c: (x, y, 1 - c))


def solution(mesh):
    def send(value, perm):
        return lax.ppermute(value, "tp", perm)

    def step(x, dy, gate, up, w_gate, w_up, w_down):
        shard, upper, lower, d_gate, d_up, hidden, block = scatter(dy, gate, up, w_gate, w_up, w_down)
        first_a, first_b = send(upper, FIRST), send(lower, FIRST)
        second = send(shard, SECOND)
        own_twin = send(shard, SIBLING)
        both_a = send(first_a, SECOND)
        both_b, both_c = send(first_b[:U], SECOND), send(first_b[U:], SECOND)
        first_a_twin, first_b_twin = send(first_a, SIBLING), send(first_b, SIBLING)
        second_twin = send(second, SIBLING)
        both_a_twin, both_b_twin = send(both_a, SIBLING), send(both_b, SIBLING)
        both_c_twin = send(both_c, SIBLING)
        wide = wide_grads(x, d_gate, d_up, 0, 3)
        dw_gate, dw_up = wide_grads(x, d_gate, d_up, 3, 3, wide)
        dw_down, dx = down_grad(
            hidden, dy, block, (shard, own_twin, first_a, first_b, second),
            ((0, 0, 0, 0, 2 * M), (1, 0, 0, 0, 2 * M), (0, 1, 0, 0, M), (0, 1, 0, M, M), (0, 0, 1, 0, 2 * M)),
        )
        dx = write(
            (first_a_twin, first_b_twin, second_twin, both_a),
            ((1, 1, 0, 0, M), (1, 1, 0, M, M), (1, 0, 1, 0, 2 * M), (0, 1, 1, 0, M)),
            dx,
        )
        dx = write(
            (both_a_twin, both_b, both_c), ((1, 1, 1, 0, M), (0, 1, 1, M, U), (0, 1, 1, M + U, U)), dx
        )
        dx = write((both_b_twin, both_c_twin), ((1, 1, 1, M, U), (1, 1, 1, M + U, U)), dx)
        return dx, dw_gate, dw_up, dw_down

    tokens, columns, rows = P("dp", None), P(None, "tp"), P("tp", None)
    return jax.shard_map(
        step,
        mesh=mesh,
        in_specs=(tokens, tokens, P("dp", "tp"), P("dp", "tp"), columns, columns, rows),
        out_specs=(tokens, P("dp", "tp"), P("dp", "tp"), P(("dp", "tp"), None)),
        check_vma=False,
    )
```

```python
import functools

import jax
import jax.numpy as jnp
from jax import lax
from jax.experimental import pallas as pl
from jax.experimental.pallas import tpu as pltpu
from jax.sharding import PartitionSpec as P


SCATTER_MIB, WIDE_MIB, DOWN_MIB = 44, 24, 24

BF16, F32 = jnp.bfloat16, jnp.float32
ROWS, D, FL = 2048, 3072, 1024
M = 256
TAIL = 64
U = M // 2
HALF = D // 2
W = 512
PIECES = HALF // W
BN = 512
EARLY = 3 * BN
LATE = (D - EARLY) // BN
STEPS = ROWS // M
ANY = pl.BlockSpec(memory_space=pl.ANY)


def nt(a, b):
    return lax.dot_general(a, b, (((1,), (1,)), ((), ())), preferred_element_type=F32)


def turned(a, b):
    return lax.dot_general(a, b, (((0,), (0,)), ((), ())), preferred_element_type=F32)


def places(parts, spots, out, sem):
    _, core, y, x = place()
    copies = []
    for k, (part, (twin, along_first, along_second, row, count)) in enumerate(zip(parts, spots)):
        half = core + twin - 2 * core * twin
        flip_y = along_first * (1 - half) + along_second * half
        flip_x = along_first * half + along_second * (1 - half)
        to_x, to_y = x + flip_x - 2 * x * flip_x, y + flip_y - 2 * y * flip_y
        cols = pl.ds(pl.multiple_of(half * HALF, HALF), HALF)
        run = TAIL if count % U else U
        for i in range(0, count, run):
            rows = pl.ds(pl.multiple_of((to_x * 2 + to_y) * 2 * M + row + i, run), run)
            copies.append(pltpu.make_async_copy(part.at[pl.ds(i, run)], out.at[rows, cols], sem.at[k, i // run]))
    return copies


def place():
    me = lax.axis_index("tp")
    core, y, x = me % 2, (me // 2) % 2, me // 4
    return me, core, y, x


def rows_of(p, x, y):
    diag, own = 1 - jnp.minimum(p // 2, 1), p // 6
    mid = 1 - diag - own
    at = diag * p * M + own * (p - 6) * M + mid * (p - 2) * U

    def run(flip_x, flip_y):
        to_x, to_y = x + flip_x - 2 * x * flip_x, y + flip_y - 2 * y * flip_y
        return (to_x * 2 + to_y) * 2 * M + at

    return run(diag, diag + mid), run(diag + mid, diag) + (1 - mid) * U


def scatter_kernel(
    dy, gate, up, w_gate, w_up, w_down,
    shard, upper, lower, d_gate, d_up, hidden, block,
    wide, wd, inb, dgb, dub, acc, sum_own,
    sib_out, sib_in, one_out, one_in, two_out, two_in,
    down_sem, wide_sem, in_sem, half_r,
    sib_s, sib_r, one_s, one_r, two_s, two_r,
):
    me, core, y, x = place()
    sibling = me + 1 - 2 * core
    near_x, near_y = me + 4 - 8 * x, me + 2 - 4 * y
    first = near_y * (1 - core) + near_x * core
    second = near_x * (1 - core) + near_y * core
    own_col, sib_col = core * HALF, (1 - core) * HALF

    def inputs(p, slot):
        made = []
        for h, row in enumerate(rows_of(p, x, y)):
            rows, at = pl.ds(pl.multiple_of(row, U), U), 0
            for far in (dy, gate, up):
                near = inb.at[slot, pl.ds(h * U, U), pl.ds(at, far.shape[1])]
                made.append(pltpu.make_async_copy(far.at[rows], near, in_sem.at[slot]))
                at += far.shape[1]
        return made

    def inputs_here(slot):
        pltpu.make_async_copy(inb.at[slot], inb.at[slot], in_sem.at[slot]).wait()

    def columns(base, j):
        return pl.ds(pl.multiple_of(base + j * W, 256), W)

    down = []
    for n in range(FL // 256):
        at = pl.ds(n * 256, 256)
        down.append(pltpu.make_async_copy(w_down.at[at], wd.at[at], down_sem.at[n]))
    slices = {}
    for j in range(PIECES):
        for side, base in ((0, sib_col), (1, own_col)):
            at = columns(base, j)
            slices[side, j] = [
                pltpu.make_async_copy(w.at[at], wide.at[k, at], wide_sem.at[side, j])
                for k, w in enumerate((w_gate, w_up))
            ]

    def remote(src, dst, send, recv, to):
        return pltpu.make_async_remote_copy(
            src_ref=src, dst_ref=dst, send_sem=send, recv_sem=recv,
            device_id={"tp": to}, device_id_type=pl.DeviceIdType.MESH,
        )

    def to_sibling(p, j):
        return remote(sib_out.at[p % 2, j], sib_in.at[p % 2, j], sib_s.at[p % 2, j], sib_r.at[p % 2, j], sibling)

    def to_first(k, j):
        return remote(one_out.at[k, j], one_in.at[k, j], one_s, one_r.at[k, j], first)

    def to_second(k, j):
        return remote(two_out.at[k, j], two_in.at[k, j], two_s, two_r.at[k, j], second)

    for c in inputs(0, 0) + down[:2]:
        c.start()

    barrier = pltpu.get_barrier_semaphore()
    for other in (sibling, first, second):
        pl.semaphore_signal(barrier, inc=1, device_id={"tp": other}, device_id_type=pl.DeviceIdType.MESH)
    pl.semaphore_wait(barrier, 3)
    for c in down[2:]:
        c.start()

    def keep(to, p, at, value):
        value = value.astype(BF16)
        for h, row in enumerate(rows_of(p, x, y)):
            to[pl.ds(pl.multiple_of(row, U), U), at] = value[h * U : (h + 1) * U]
        return value

    def hidden_grads(p, slot, n):
        at = slice(n * 256, (n + 1) * 256)
        d_hidden = nt(inb[slot, :, :D], wd[at, :])
        g = inb[slot, :, D + n * 256 : D + (n + 1) * 256].astype(F32)
        u = inb[slot, :, D + FL + n * 256 : D + FL + (n + 1) * 256].astype(F32)
        s = jax.nn.sigmoid(g)
        act = g * s
        keep(hidden, p, at, act * u)
        dub[:, at] = keep(d_up, p, at, d_hidden * act)
        dgb[:, at] = keep(d_gate, p, at, d_hidden * u * (s + act * (1 - s)))

    def term(base, j):
        at = columns(base, j)
        return (nt(dgb[...], wide[0, at, :]) + nt(dub[...], wide[1, at, :])).reshape(2, U, W)

    def for_sibling(p, pieces):
        for j in pieces:
            sib_out[p % 2, j] = term(sib_col, j).astype(BF16)
        for j in pieces:
            to_sibling(p, j).start()

    def chip_sum(p, j, h):
        return acc[j, h] + sib_in[p % 2, j, h].astype(F32)

    def send_diagonal(p, j):
        for h in range(2):
            one_out[2 * p + h, j] = chip_sum(p, j, h).astype(BF16)
            to_first(2 * p + h, j).start()

    def send_middle(p):
        q = p - 2
        for j in range(PIECES):
            to_sibling(p, j).wait_recv()
            one_out[4 + q, j] = chip_sum(p, j, core).astype(BF16)
            to_first(4 + q, j).start()
        for j in range(PIECES):
            to_first(q, j).wait_recv()
            two_out[q, j] = (chip_sum(p, j, 1 - core) + one_in[q, j].astype(F32)).astype(BF16)
            to_second(q, j).start()

    def keep_own(p):
        for j in range(PIECES):
            to_sibling(p, j).wait_recv()
            for h in range(2):
                sum_own[2 * (p - 6) + h, j] = chip_sum(p, j, h)

    def diagonal_step(p, ready, done):
        for j in range(done, PIECES + 1):
            if done + (done > 0) <= j < PIECES:
                ready(0, j)
                for_sibling(p, (j,))
            if j > done:
                ready(1, j - 1)
                acc[j - 1] = term(own_col, j - 1)
                to_sibling(p, j - 1).wait_recv()
                send_diagonal(p, j - 1)

    def arrived(side, j):
        here = wide.at[:, columns((sib_col, own_col)[side], j)]
        pltpu.make_async_copy(here, here, wide_sem.at[side, j]).wait()

    down_inputs = []
    for k in range(ROWS // FL):
        near = wd.at[:, pl.ds(k * EARLY, EARLY)]
        down_inputs.append(pltpu.make_async_copy(dy.at[pl.ds(k * FL, FL), pl.ds(0, EARLY)], near, down_sem.at[k]))

    def first_piece():
        halves = [pl.ds(i * (W // 2), W // 2) for i in range(2)]

        def copy(i):
            a, b = sib_out.at[0, 0, :, :, halves[i]], sib_in.at[0, 0, :, :, halves[i]]
            return remote(a, b, sib_s.at[0, 0], half_r.at[i], sibling)

        for i in range(2):
            for side, base in enumerate((sib_col, own_col)):
                if i == 0:
                    arrived(side, 0)
                at = pl.ds(pl.multiple_of(base + i * (W // 2), 256), W // 2)
                part = (nt(dgb[...], wide[0, at, :]) + nt(dub[...], wide[1, at, :])).reshape(2, U, W // 2)
                if side:
                    acc[0, :, :, halves[i]] = part
                else:
                    sib_out[0, 0, :, :, halves[i]] = part.astype(BF16)
                    copy(i).start()
        for i in range(2):
            copy(i).wait_recv()
            for h in range(2):
                total = acc[0, h, :, halves[i]] + sib_in[0, 0, h, :, halves[i]].astype(F32)
                one_out[h, 0, :, halves[i]] = total.astype(BF16)
                a, b = one_out.at[h, 0, :, halves[i]], one_in.at[h, 0, :, halves[i]]
                remote(a, b, one_s, one_r.at[h, 0], first).start()
            if i == 0:
                arrived(0, 1)
                for_sibling(0, (1,))

    inputs_here(0)
    for c in down[:2]:
        c.wait()
    for c in slices[0, 0] + slices[1, 0]:
        c.start()
    for n in range(2):
        hidden_grads(0, 0, n)
    for c in down[2:]:
        c.wait()
    for k in ((0, 1), (0, 2), (1, 1), (1, 2)):
        for c in slices[k]:
            c.start()
    for c in inputs(1, 1):
        c.start()
    for n in range(2, 4):
        hidden_grads(0, 0, n)
    first_piece()
    diagonal_step(0, arrived, 1)
    inputs_here(1)
    for c in inputs(2, 0):
        c.start()
    for n in range(FL // 256):
        hidden_grads(1, 1, n)
    diagonal_step(1, lambda side, j: None, 0)

    def step(p, carry):
        slot = p % 2
        inputs_here(slot)

        @pl.when(p < STEPS - 1)
        def _():
            for c in inputs(p + 1, 1 - slot):
                c.start()

        for n in range(FL // 256):
            hidden_grads(p, slot, n)

        @pl.when(jnp.logical_and(p >= 4, p < 7))
        def _():
            send_middle(p - 1)

        @pl.when(p == 7)
        def _():
            for c in down_inputs:
                c.start()
            keep_own(6)

        for j in range(PIECES):
            to_sibling(p, j).wait_send()
        for_sibling(p, range(PIECES))
        for j in range(PIECES):
            acc[j] = term(own_col, j)

        @pl.when(p == 2)
        def _():
            send_middle(2)

        return carry

    lax.fori_loop(2, STEPS, step, 0)
    keep_own(STEPS - 1)

    for c in down_inputs:
        c.wait()
    for n in range(0, EARLY, 256):
        right = jnp.concatenate([wd[:, pl.ds(k * EARLY + n, 256)] for k in range(ROWS // FL)])
        block[:, pl.ds(n, 256)] = turned(hidden[...], right).astype(BF16)

    for q in range(4):
        for j in range(PIECES):
            to_first(4 + q, j).wait_recv()
            to_second(q, j).wait_recv()
            total = sum_own[q, j] + one_in[4 + q, j].astype(F32) + two_in[q, j].astype(F32)
            for to, row in ((upper, lower)[q // 2], q % 2), (shard, q):
                to[pl.ds(row * U, U), pl.ds(j * W, W)] = total.astype(BF16)
    for p in (STEPS - 2, STEPS - 1):
        for j in range(PIECES):
            to_sibling(p, j).wait_send()
    remote(one_out, one_in, one_s, one_r.at[0, 0], first).wait_send()
    remote(two_out, two_in, two_s, two_r.at[0, 0], second).wait_send()


def scatter(dy, gate, up, w_gate, w_up, w_down):
    dma = pltpu.SemaphoreType.DMA
    hid, part = pltpu.VMEM((ROWS, FL), BF16), pltpu.VMEM((M, HALF), BF16)
    units = lambda n: pltpu.VMEM((n, PIECES, U, W), BF16)
    twin = pltpu.VMEM((2, PIECES, 2, U, W), BF16)
    return pl.pallas_call(
        scatter_kernel,
        out_shape=(pltpu.VMEM((2 * M, HALF), BF16), part, part, hid, hid, hid, pltpu.VMEM((FL, EARLY), BF16)),
        in_specs=[ANY] * 6,
        out_specs=(pl.BlockSpec(memory_space=pltpu.VMEM),) * 7,
        scratch_shapes=[
            pltpu.VMEM((2, D, FL), BF16), pltpu.VMEM((FL, D), BF16), pltpu.VMEM((2, M, D + 2 * FL), BF16),
            pltpu.VMEM((M, FL), BF16), pltpu.VMEM((M, FL), BF16),
            pltpu.VMEM((PIECES, 2, U, W), F32), pltpu.VMEM((4, PIECES, U, W), F32),
            twin, twin, units(8), units(8), units(4), units(4),
            dma((FL // 256,)), dma((2, PIECES)), dma((2,)), dma((2,)),
            dma((2, PIECES)), dma((2, PIECES)), dma, dma((8, PIECES)), dma, dma((4, PIECES)),
        ],
        compiler_params=pltpu.CompilerParams(
            collective_id=0, has_side_effects=True, vmem_limit_bytes=SCATTER_MIB * 2**20
        ),
        cost_estimate=pl.CostEstimate(
            flops=6 * ROWS * D * FL, bytes_accessed=60 * 2**20, transcendentals=2 * ROWS * FL
        ),
        name="scatter",
    )(dy, gate, up, w_gate, w_up, w_down)


def placed(value, space):
    return pltpu.with_memory_space_constraint(value, space)


def streamed(far, near, sem, start, first, use):
    step, count = pl.program_id(0), pl.num_programs(0)

    def fetch(i):
        cols = pl.ds(pl.multiple_of((start + i) * BN, BN), BN)
        return pltpu.make_async_copy(far.at[:, cols], near.at[i % 2], sem.at[i % 2])

    if first is None:

        @pl.when(step == 0)
        def _():
            fetch(0).start()

        fetch(step).wait()

    @pl.when(step + 1 < count)
    def _():
        fetch(step + 1).start()

    if first is None:
        use(near.at[step % 2])
    else:

        @pl.when(step == 0)
        def _():
            use(first)

        @pl.when(step > 0)
        def _():
            fetch(step).wait()
            use(near.at[step % 2])


def wide_kernel(start, after, given, x, d_gate, d_up, further, *refs):
    first = refs[0] if given else None
    dw_gate, dw_up, ahead, near, sem, ahead_sem = refs[-6:]
    step, last = pl.program_id(0), pl.num_programs(0) - 1
    fetch = pltpu.make_async_copy(further.at[:, pl.ds(after * BN, BN)], ahead, ahead_sem)

    def use(block):
        xt = block[...].T
        dw_gate[...] = jnp.dot(xt, d_gate[...], preferred_element_type=F32).astype(BF16)
        dw_up[...] = jnp.dot(xt, d_up[...], preferred_element_type=F32).astype(BF16)

    streamed(x, near, sem, start, first, use)

    @pl.when(step == 0)
    def _():
        fetch.start()

    @pl.when(step == last)
    def _():
        fetch.wait()


def wide_grads(x, d_gate, d_up, start, count, further, after, first=None, into=()):
    whole = pl.BlockSpec((ROWS, FL), lambda i: (0, 0), pipeline_mode=pl.Buffered(1))
    block = pl.BlockSpec((ROWS, BN), lambda i: (0, 0), pipeline_mode=pl.Buffered(1))
    out = pl.BlockSpec((BN, FL), lambda i: (start + i, 0))
    shape = jax.ShapeDtypeStruct((D, FL), BF16)
    dma = pltpu.SemaphoreType.DMA
    given = () if first is None else (placed(first, pltpu.VMEM),)
    return pl.pallas_call(
        functools.partial(wide_kernel, start, after, bool(given)),
        grid=(count,),
        out_shape=(shape, shape, pltpu.VMEM((ROWS, BN), BF16)),
        in_specs=[ANY, whole, whole, ANY] + [block] * len(given) + [ANY] * len(into),
        out_specs=(out, out, ANY),
        scratch_shapes=[pltpu.VMEM((2, ROWS, BN), BF16), dma((2,)), dma],
        input_output_aliases={4 + len(given) + k: k for k in range(len(into))},
        compiler_params=pltpu.CompilerParams(vmem_limit_bytes=WIDE_MIB * 2**20),
        cost_estimate=pl.CostEstimate(flops=4 * ROWS * BN * count * FL, bytes_accessed=20 * 2**20, transcendentals=0),
        name="wide_grads",
    )(
        placed(x, pltpu.HBM), placed(d_gate, pltpu.VMEM), placed(d_up, pltpu.VMEM), placed(further, pltpu.HBM),
        *given, *into,
    )


def down_kernel(spots, hidden, dy, block, first, *refs):
    n = len(spots)
    parts, (out, dx, made, near, part_sem, block_sem, made_sem, sem) = refs[:n], refs[n:]
    step, last = pl.program_id(0), pl.num_programs(0) - 1

    def save(i):
        cols = pl.ds(pl.multiple_of(EARLY + i * BN, BN), BN)
        return pltpu.make_async_copy(made.at[i % 2], out.at[:, cols], made_sem.at[i % 2])

    early = pltpu.make_async_copy(block, out.at[:, pl.ds(0, EARLY)], block_sem)

    @pl.when(step >= 2)
    def _():
        save(step - 2).wait()

    def use(right):
        made[step % 2] = turned(hidden[...], right[...]).astype(BF16)

    streamed(dy, near, sem, EARLY // BN, first, use)
    save(step).start()

    @pl.when(step == 0)
    def _():
        early.start()
        for c in places(parts, spots, dx, part_sem):
            c.start()

    @pl.when(step == last)
    def _():
        early.wait()
        for c in places(parts, spots, dx, part_sem):
            c.wait()
        save(step - 1).wait()
        save(step).wait()


def down_grad(hidden, dy, block, first, parts, spots):
    n = len(parts)
    dma = pltpu.SemaphoreType.DMA
    whole = lambda *shape: pl.BlockSpec(shape, lambda i: (0, 0), pipeline_mode=pl.Buffered(1))
    return pl.pallas_call(
        functools.partial(down_kernel, spots),
        grid=(LATE,),
        out_shape=(jax.ShapeDtypeStruct((FL, D), BF16), jax.ShapeDtypeStruct((ROWS, D), BF16)),
        in_specs=[whole(ROWS, FL), ANY, whole(FL, EARLY), whole(ROWS, BN)] + [ANY] * n,
        out_specs=(ANY, ANY),
        scratch_shapes=[
            pltpu.VMEM((2, FL, BN), BF16), pltpu.VMEM((2, ROWS, BN), BF16),
            dma((n, 2 * M // U)), dma, dma((2,)), dma((2,)),
        ],
        compiler_params=pltpu.CompilerParams(vmem_limit_bytes=DOWN_MIB * 2**20),
        cost_estimate=pl.CostEstimate(flops=2 * ROWS * D * FL, bytes_accessed=24 * 2**20, transcendentals=0),
        name="down_grad",
    )(
        placed(hidden, pltpu.VMEM), placed(dy, pltpu.HBM), placed(block, pltpu.VMEM), placed(first, pltpu.VMEM),
        *parts,
    )


def write_kernel(spots, *refs):
    copies = places(refs[: len(spots)], spots, refs[-2], refs[-1])
    for c in copies:
        c.start()
    for c in copies:
        c.wait()


def write(parts, spots, into=None):
    n = len(parts)
    given = () if into is None else (into,)
    return pl.pallas_call(
        functools.partial(write_kernel, spots),
        out_shape=jax.ShapeDtypeStruct((ROWS, D), BF16),
        in_specs=[pl.BlockSpec(memory_space=pltpu.VMEM)] * n + [ANY] * len(given),
        out_specs=ANY,
        scratch_shapes=[pltpu.SemaphoreType.DMA((n, 2 * M // U))],
        input_output_aliases={n: 0} if given else {},
        compiler_params=pltpu.CompilerParams(vmem_limit_bytes=16 * 1024 * 1024),
        cost_estimate=pl.CostEstimate(flops=10**9, bytes_accessed=24 * 2**20, transcendentals=0),
        name="write",
    )(*parts, *given)


def index(x, y, core):
    return (x * 2 + y) * 2 + core


def pairs(to):
    return [(index(x, y, c), index(*to(x, y, c))) for x in (0, 1) for y in (0, 1) for c in (0, 1)]


FIRST = pairs(lambda x, y, c: (x, 1 - y, c) if c == 0 else (1 - x, y, c))
SECOND = pairs(lambda x, y, c: (1 - x, y, c) if c == 0 else (x, 1 - y, c))
SIBLING = pairs(lambda x, y, c: (x, y, 1 - c))


def solution(mesh):
    def send(value, perm):
        return lax.ppermute(value, "tp", perm)

    def step(x, dy, gate, up, w_gate, w_up, w_down):
        shard, upper, lower, d_gate, d_up, hidden, block = scatter(dy, gate, up, w_gate, w_up, w_down)
        first_a, first_b = send(upper, FIRST), send(lower, FIRST)
        second = send(shard, SECOND)
        own_twin = send(shard, SIBLING)
        both_a = send(first_a, SECOND)
        both_b, both_c = send(first_b[: M - TAIL], SECOND), send(first_b[M - TAIL :], SECOND)
        first_a_twin, first_b_twin = send(first_a, SIBLING), send(first_b, SIBLING)
        second_twin = send(second, SIBLING)
        both_a_twin, both_b_twin = send(both_a, SIBLING), send(both_b, SIBLING)
        both_c_twin = send(both_c, SIBLING)
        *wide, ahead = wide_grads(x, d_gate, d_up, 0, 3, x, 3)
        dw_gate, dw_up, ahead = wide_grads(x, d_gate, d_up, 3, 3, dy, EARLY // BN, ahead, wide)
        dw_down, dx = down_grad(
            hidden, dy, block, ahead, (shard, own_twin, first_a, first_b, second),
            ((0, 0, 0, 0, 2 * M), (1, 0, 0, 0, 2 * M), (0, 1, 0, 0, M), (0, 1, 0, M, M), (0, 0, 1, 0, 2 * M)),
        )
        dx = write(
            (first_a_twin, first_b_twin, second_twin, both_a),
            ((1, 1, 0, 0, M), (1, 1, 0, M, M), (1, 0, 1, 0, 2 * M), (0, 1, 1, 0, M)),
            dx,
        )
        dx = write((both_a_twin, both_b), ((1, 1, 1, 0, M), (0, 1, 1, M, M - TAIL)), dx)
        dx = write(
            (both_b_twin, both_c, both_c_twin),
            ((1, 1, 1, M, M - TAIL), (0, 1, 1, 2 * M - TAIL, TAIL), (1, 1, 1, 2 * M - TAIL, TAIL)),
            dx,
        )
        return dx, dw_gate, dw_up, dw_down

    tokens, columns, rows = P("dp", None), P(None, "tp"), P("tp", None)
    return jax.shard_map(
        step,
        mesh=mesh,
        in_specs=(tokens, tokens, P("dp", "tp"), P("dp", "tp"), columns, columns, rows),
        out_specs=(tokens, P("dp", "tp"), P("dp", "tp"), P(("dp", "tp"), None)),
        check_vma=False,
    )
```

```python
import functools

import jax
import jax.numpy as jnp
from jax import lax
from jax.experimental import pallas as pl
from jax.experimental.pallas import tpu as pltpu
from jax.sharding import PartitionSpec as P


SCATTER_MIB, WIDE_MIB, DOWN_MIB = 44, 24, 24

BF16, F32 = jnp.bfloat16, jnp.float32
ROWS, D, FL = 2048, 3072, 1024
M = 256
TAIL = 64
U = M // 2
HALF = D // 2
W = 512
PIECES = HALF // W
BN = 512
EARLY = 3 * BN
LATE = (D - EARLY) // BN
STEPS = ROWS // M
ANY = pl.BlockSpec(memory_space=pl.ANY)


def nt(a, b):
    return lax.dot_general(a, b, (((1,), (1,)), ((), ())), preferred_element_type=F32)


def turned(a, b):
    return lax.dot_general(a, b, (((0,), (0,)), ((), ())), preferred_element_type=F32)


def places(parts, spots, out, sem):
    _, core, y, x = place()
    copies = []
    for k, (part, (twin, along_first, along_second, row, count)) in enumerate(zip(parts, spots)):
        half = core + twin - 2 * core * twin
        flip_y = along_first * (1 - half) + along_second * half
        flip_x = along_first * half + along_second * (1 - half)
        to_x, to_y = x + flip_x - 2 * x * flip_x, y + flip_y - 2 * y * flip_y
        cols = pl.ds(pl.multiple_of(half * HALF, HALF), HALF)
        run = TAIL if count % U else U
        for i in range(0, count, run):
            rows = pl.ds(pl.multiple_of((to_x * 2 + to_y) * 2 * M + row + i, run), run)
            copies.append(pltpu.make_async_copy(part.at[pl.ds(i, run)], out.at[rows, cols], sem.at[k, i // run]))
    return copies


def place():
    me = lax.axis_index("tp")
    core, y, x = me % 2, (me // 2) % 2, me // 4
    return me, core, y, x


def rows_of(p, x, y):
    diag, own = 1 - jnp.minimum(p // 2, 1), p // 6
    mid = 1 - diag - own
    at = diag * p * M + own * (p - 6) * M + mid * (p - 2) * U

    def run(flip_x, flip_y):
        to_x, to_y = x + flip_x - 2 * x * flip_x, y + flip_y - 2 * y * flip_y
        return (to_x * 2 + to_y) * 2 * M + at

    return run(diag, diag + mid), run(diag + mid, diag) + (1 - mid) * U


def scatter_kernel(
    dy, gate, up, w_gate, w_up, w_down,
    shard, upper, lower, d_gate, d_up, hidden, block,
    wide, wd, inb, dgb, dub, acc, sum_own,
    sib_out, sib_in, one_out, one_in, two_out, two_in,
    down_sem, wide_sem, in_sem, half_r,
    sib_s, sib_r, one_s, one_r, two_s, two_r,
):
    me, core, y, x = place()
    sibling = me + 1 - 2 * core
    near_x, near_y = me + 4 - 8 * x, me + 2 - 4 * y
    first = near_y * (1 - core) + near_x * core
    second = near_x * (1 - core) + near_y * core
    own_col, sib_col = core * HALF, (1 - core) * HALF

    def inputs(p, slot):
        made = []
        for h, row in enumerate(rows_of(p, x, y)):
            rows, at = pl.ds(pl.multiple_of(row, U), U), 0
            for far in (dy, gate, up):
                near = inb.at[slot, pl.ds(h * U, U), pl.ds(at, far.shape[1])]
                made.append(pltpu.make_async_copy(far.at[rows], near, in_sem.at[slot]))
                at += far.shape[1]
        return made

    def inputs_here(slot):
        pltpu.make_async_copy(inb.at[slot], inb.at[slot], in_sem.at[slot]).wait()

    def columns(base, j):
        return pl.ds(pl.multiple_of(base + j * W, 256), W)

    down = []
    for n in range(FL // 256):
        at = pl.ds(n * 256, 256)
        down.append(pltpu.make_async_copy(w_down.at[at], wd.at[at], down_sem.at[n]))
    slices = {}
    for j in range(PIECES):
        for side, base in ((0, sib_col), (1, own_col)):
            at = columns(base, j)
            slices[side, j] = [
                pltpu.make_async_copy(w.at[at], wide.at[k, at], wide_sem.at[side, j])
                for k, w in enumerate((w_gate, w_up))
            ]

    def remote(src, dst, send, recv, to):
        return pltpu.make_async_remote_copy(
            src_ref=src, dst_ref=dst, send_sem=send, recv_sem=recv,
            device_id={"tp": to}, device_id_type=pl.DeviceIdType.MESH,
        )

    def to_sibling(p, j):
        return remote(sib_out.at[p % 2, j], sib_in.at[p % 2, j], sib_s.at[p % 2, j], sib_r.at[p % 2, j], sibling)

    def to_first(k, j):
        return remote(one_out.at[k, j], one_in.at[k, j], one_s, one_r.at[k], first)

    def unit_here(into, sems, k):
        pltpu.make_async_copy(into.at[k], into.at[k], sems.at[k]).wait()

    def to_second(k, j):
        return remote(two_out.at[k, j], two_in.at[k, j], two_s, two_r.at[k], second)

    for c in inputs(0, 0) + down[:2]:
        c.start()

    barrier = pltpu.get_barrier_semaphore()
    for other in (sibling, first, second):
        pl.semaphore_signal(barrier, inc=1, device_id={"tp": other}, device_id_type=pl.DeviceIdType.MESH)
    pl.semaphore_wait(barrier, 3)
    for c in down[2:]:
        c.start()

    def keep(to, p, at, value):
        value = value.astype(BF16)
        for h, row in enumerate(rows_of(p, x, y)):
            to[pl.ds(pl.multiple_of(row, U), U), at] = value[h * U : (h + 1) * U]
        return value

    def hidden_grads(p, slot, n):
        at = slice(n * 256, (n + 1) * 256)
        d_hidden = nt(inb[slot, :, :D], wd[at, :])
        g = inb[slot, :, D + n * 256 : D + (n + 1) * 256].astype(F32)
        u = inb[slot, :, D + FL + n * 256 : D + FL + (n + 1) * 256].astype(F32)
        s = jax.nn.sigmoid(g)
        act = g * s
        keep(hidden, p, at, act * u)
        dub[:, at] = keep(d_up, p, at, d_hidden * act)
        dgb[:, at] = keep(d_gate, p, at, d_hidden * u * (s + act * (1 - s)))

    def term(base, j):
        at = columns(base, j)
        return (nt(dgb[...], wide[0, at, :]) + nt(dub[...], wide[1, at, :])).reshape(2, U, W)

    def for_sibling(p, pieces):
        for j in pieces:
            sib_out[p % 2, j] = term(sib_col, j).astype(BF16)
        for j in pieces:
            to_sibling(p, j).start()

    def chip_sum(p, j, h):
        return acc[j, h] + sib_in[p % 2, j, h].astype(F32)

    def send_diagonal(p, j):
        for h in range(2):
            one_out[2 * p + h, j] = chip_sum(p, j, h).astype(BF16)
            to_first(2 * p + h, j).start()

    def send_middle(p):
        q = p - 2
        for j in range(PIECES):
            to_sibling(p, j).wait_recv()
            one_out[4 + q, j] = chip_sum(p, j, core).astype(BF16)
            to_first(4 + q, j).start()
        unit_here(one_in, one_r, q)
        for j in range(PIECES):
            two_out[q, j] = (chip_sum(p, j, 1 - core) + one_in[q, j].astype(F32)).astype(BF16)
            to_second(q, j).start()

    def keep_own(p):
        for j in range(PIECES):
            to_sibling(p, j).wait_recv()
            for h in range(2):
                sum_own[2 * (p - 6) + h, j] = chip_sum(p, j, h)

    def diagonal_step(p, ready, done):
        for j in range(done, PIECES + 1):
            if done + (done > 0) <= j < PIECES:
                ready(0, j)
                for_sibling(p, (j,))
            if j > done:
                ready(1, j - 1)
                acc[j - 1] = term(own_col, j - 1)
                to_sibling(p, j - 1).wait_recv()
                send_diagonal(p, j - 1)

    def arrived(side, j):
        here = wide.at[:, columns((sib_col, own_col)[side], j)]
        pltpu.make_async_copy(here, here, wide_sem.at[side, j]).wait()

    down_inputs = []
    for k in range(ROWS // FL):
        near = wd.at[:, pl.ds(k * EARLY, EARLY)]
        down_inputs.append(pltpu.make_async_copy(dy.at[pl.ds(k * FL, FL), pl.ds(0, EARLY)], near, down_sem.at[k]))

    def first_piece():
        halves = [pl.ds(i * (W // 2), W // 2) for i in range(2)]

        def copy(i):
            a, b = sib_out.at[0, 0, :, :, halves[i]], sib_in.at[0, 0, :, :, halves[i]]
            return remote(a, b, sib_s.at[0, 0], half_r.at[i], sibling)

        for i in range(2):
            for side, base in enumerate((sib_col, own_col)):
                if i == 0:
                    arrived(side, 0)
                at = pl.ds(pl.multiple_of(base + i * (W // 2), 256), W // 2)
                part = (nt(dgb[...], wide[0, at, :]) + nt(dub[...], wide[1, at, :])).reshape(2, U, W // 2)
                if side:
                    acc[0, :, :, halves[i]] = part
                else:
                    sib_out[0, 0, :, :, halves[i]] = part.astype(BF16)
                    copy(i).start()
        for i in range(2):
            copy(i).wait_recv()
            for h in range(2):
                total = acc[0, h, :, halves[i]] + sib_in[0, 0, h, :, halves[i]].astype(F32)
                one_out[h, 0, :, halves[i]] = total.astype(BF16)
                a, b = one_out.at[h, 0, :, halves[i]], one_in.at[h, 0, :, halves[i]]
                remote(a, b, one_s, one_r.at[h], first).start()
            if i == 0:
                arrived(0, 1)
                for_sibling(0, (1,))

    inputs_here(0)
    for c in down[:2]:
        c.wait()
    for c in slices[0, 0] + slices[1, 0]:
        c.start()
    for n in range(2):
        hidden_grads(0, 0, n)
    for c in down[2:]:
        c.wait()
    for k in ((0, 1), (0, 2), (1, 1), (1, 2)):
        for c in slices[k]:
            c.start()
    for c in inputs(1, 1):
        c.start()
    for n in range(2, 4):
        hidden_grads(0, 0, n)
    first_piece()
    diagonal_step(0, arrived, 1)
    inputs_here(1)
    for c in inputs(2, 0):
        c.start()
    for n in range(FL // 256):
        hidden_grads(1, 1, n)
    diagonal_step(1, lambda side, j: None, 0)

    def step(p, carry):
        slot = p % 2
        inputs_here(slot)

        @pl.when(p < STEPS - 1)
        def _():
            for c in inputs(p + 1, 1 - slot):
                c.start()

        for n in range(FL // 256):
            hidden_grads(p, slot, n)

        @pl.when(jnp.logical_and(p >= 5, p < 7))
        def _():
            send_middle(p - 1)

        @pl.when(p == 7)
        def _():
            for c in down_inputs:
                c.start()
            keep_own(6)

        for j in range(PIECES):
            to_sibling(p, j).wait_send()
        for_sibling(p, range(PIECES))
        for j in range(PIECES):
            acc[j] = term(own_col, j)

        @pl.when(p < 4)
        def _():
            send_middle(p)

        return carry

    lax.fori_loop(2, STEPS, step, 0)
    keep_own(STEPS - 1)

    for c in down_inputs:
        c.wait()
    for n in range(0, EARLY, 256):
        right = jnp.concatenate([wd[:, pl.ds(k * EARLY + n, 256)] for k in range(ROWS // FL)])
        block[:, pl.ds(n, 256)] = turned(hidden[...], right).astype(BF16)

    for q in range(4):
        unit_here(one_in, one_r, 4 + q)
        unit_here(two_in, two_r, q)
        for j in range(PIECES):
            total = sum_own[q, j] + one_in[4 + q, j].astype(F32) + two_in[q, j].astype(F32)
            for to, row in ((upper, lower)[q // 2], q % 2), (shard, q):
                to[pl.ds(row * U, U), pl.ds(j * W, W)] = total.astype(BF16)
    for p in (STEPS - 2, STEPS - 1):
        for j in range(PIECES):
            to_sibling(p, j).wait_send()
    remote(one_out, one_in, one_s, one_r.at[0], first).wait_send()
    remote(two_out, two_in, two_s, two_r.at[0], second).wait_send()


def scatter(dy, gate, up, w_gate, w_up, w_down):
    dma = pltpu.SemaphoreType.DMA
    hid, part = pltpu.VMEM((ROWS, FL), BF16), pltpu.VMEM((M, HALF), BF16)
    units = lambda n: pltpu.VMEM((n, PIECES, U, W), BF16)
    twin = pltpu.VMEM((2, PIECES, 2, U, W), BF16)
    return pl.pallas_call(
        scatter_kernel,
        out_shape=(pltpu.VMEM((2 * M, HALF), BF16), part, part, hid, hid, hid, pltpu.VMEM((FL, EARLY), BF16)),
        in_specs=[ANY] * 6,
        out_specs=(pl.BlockSpec(memory_space=pltpu.VMEM),) * 7,
        scratch_shapes=[
            pltpu.VMEM((2, D, FL), BF16), pltpu.VMEM((FL, D), BF16), pltpu.VMEM((2, M, D + 2 * FL), BF16),
            pltpu.VMEM((M, FL), BF16), pltpu.VMEM((M, FL), BF16),
            pltpu.VMEM((PIECES, 2, U, W), F32), pltpu.VMEM((4, PIECES, U, W), F32),
            twin, twin, units(8), units(8), units(4), units(4),
            dma((FL // 256,)), dma((2, PIECES)), dma((2,)), dma((2,)),
            dma((2, PIECES)), dma((2, PIECES)), dma, dma((8,)), dma, dma((4,)),
        ],
        compiler_params=pltpu.CompilerParams(
            collective_id=0, has_side_effects=True, vmem_limit_bytes=SCATTER_MIB * 2**20
        ),
        cost_estimate=pl.CostEstimate(
            flops=6 * ROWS * D * FL, bytes_accessed=60 * 2**20, transcendentals=2 * ROWS * FL
        ),
        name="scatter",
    )(dy, gate, up, w_gate, w_up, w_down)


def placed(value, space):
    return pltpu.with_memory_space_constraint(value, space)


def streamed(far, near, sem, start, first, use):
    step, count = pl.program_id(0), pl.num_programs(0)

    def fetch(i):
        cols = pl.ds(pl.multiple_of((start + i) * BN, BN), BN)
        return pltpu.make_async_copy(far.at[:, cols], near.at[i % 2], sem.at[i % 2])

    if first is None:

        @pl.when(step == 0)
        def _():
            fetch(0).start()

        fetch(step).wait()

    @pl.when(step + 1 < count)
    def _():
        fetch(step + 1).start()

    if first is None:
        use(near.at[step % 2])
    else:

        @pl.when(step == 0)
        def _():
            use(first)

        @pl.when(step > 0)
        def _():
            fetch(step).wait()
            use(near.at[step % 2])


def wide_kernel(start, after, given, x, d_gate, d_up, further, *refs):
    first = refs[0] if given else None
    dw_gate, dw_up, ahead, near, sem, ahead_sem = refs[-6:]
    step, last = pl.program_id(0), pl.num_programs(0) - 1
    fetch = pltpu.make_async_copy(further.at[:, pl.ds(after * BN, BN)], ahead, ahead_sem)

    def use(block):
        xt = block[...].T
        dw_gate[...] = jnp.dot(xt, d_gate[...], preferred_element_type=F32).astype(BF16)
        dw_up[...] = jnp.dot(xt, d_up[...], preferred_element_type=F32).astype(BF16)

    streamed(x, near, sem, start, first, use)

    @pl.when(step == 0)
    def _():
        fetch.start()

    @pl.when(step == last)
    def _():
        fetch.wait()


def wide_grads(x, d_gate, d_up, start, count, further, after, first=None, into=()):
    whole = pl.BlockSpec((ROWS, FL), lambda i: (0, 0), pipeline_mode=pl.Buffered(1))
    block = pl.BlockSpec((ROWS, BN), lambda i: (0, 0), pipeline_mode=pl.Buffered(1))
    out = pl.BlockSpec((BN, FL), lambda i: (start + i, 0))
    shape = jax.ShapeDtypeStruct((D, FL), BF16)
    dma = pltpu.SemaphoreType.DMA
    given = () if first is None else (placed(first, pltpu.VMEM),)
    return pl.pallas_call(
        functools.partial(wide_kernel, start, after, bool(given)),
        grid=(count,),
        out_shape=(shape, shape, pltpu.VMEM((ROWS, BN), BF16)),
        in_specs=[ANY, whole, whole, ANY] + [block] * len(given) + [ANY] * len(into),
        out_specs=(out, out, ANY),
        scratch_shapes=[pltpu.VMEM((2, ROWS, BN), BF16), dma((2,)), dma],
        input_output_aliases={4 + len(given) + k: k for k in range(len(into))},
        compiler_params=pltpu.CompilerParams(vmem_limit_bytes=WIDE_MIB * 2**20),
        cost_estimate=pl.CostEstimate(flops=4 * ROWS * BN * count * FL, bytes_accessed=20 * 2**20, transcendentals=0),
        name="wide_grads",
    )(
        placed(x, pltpu.HBM), placed(d_gate, pltpu.VMEM), placed(d_up, pltpu.VMEM), placed(further, pltpu.HBM),
        *given, *into,
    )


def down_kernel(spots, hidden, dy, block, first, *refs):
    n = len(spots)
    parts, (out, dx, made, near, part_sem, block_sem, made_sem, sem) = refs[:n], refs[n:]
    step, last = pl.program_id(0), pl.num_programs(0) - 1

    def save(i):
        cols = pl.ds(pl.multiple_of(EARLY + i * BN, BN), BN)
        return pltpu.make_async_copy(made.at[i % 2], out.at[:, cols], made_sem.at[i % 2])

    early = pltpu.make_async_copy(block, out.at[:, pl.ds(0, EARLY)], block_sem)

    @pl.when(step >= 2)
    def _():
        save(step - 2).wait()

    def use(right):
        made[step % 2] = turned(hidden[...], right[...]).astype(BF16)

    streamed(dy, near, sem, EARLY // BN, first, use)
    save(step).start()

    @pl.when(step == 0)
    def _():
        early.start()
        for c in places(parts, spots, dx, part_sem):
            c.start()

    @pl.when(step == last)
    def _():
        early.wait()
        for c in places(parts, spots, dx, part_sem):
            c.wait()
        save(step - 1).wait()
        save(step).wait()


def down_grad(hidden, dy, block, first, parts, spots):
    n = len(parts)
    dma = pltpu.SemaphoreType.DMA
    whole = lambda *shape: pl.BlockSpec(shape, lambda i: (0, 0), pipeline_mode=pl.Buffered(1))
    return pl.pallas_call(
        functools.partial(down_kernel, spots),
        grid=(LATE,),
        out_shape=(jax.ShapeDtypeStruct((FL, D), BF16), jax.ShapeDtypeStruct((ROWS, D), BF16)),
        in_specs=[whole(ROWS, FL), ANY, whole(FL, EARLY), whole(ROWS, BN)] + [ANY] * n,
        out_specs=(ANY, ANY),
        scratch_shapes=[
            pltpu.VMEM((2, FL, BN), BF16), pltpu.VMEM((2, ROWS, BN), BF16),
            dma((n, 2 * M // U)), dma, dma((2,)), dma((2,)),
        ],
        compiler_params=pltpu.CompilerParams(vmem_limit_bytes=DOWN_MIB * 2**20),
        cost_estimate=pl.CostEstimate(flops=2 * ROWS * D * FL, bytes_accessed=24 * 2**20, transcendentals=0),
        name="down_grad",
    )(
        placed(hidden, pltpu.VMEM), placed(dy, pltpu.HBM), placed(block, pltpu.VMEM), placed(first, pltpu.VMEM),
        *parts,
    )


def write_kernel(spots, *refs):
    copies = places(refs[: len(spots)], spots, refs[-2], refs[-1])
    for c in copies:
        c.start()
    for c in copies:
        c.wait()


def write(parts, spots, into=None):
    n = len(parts)
    given = () if into is None else (into,)
    return pl.pallas_call(
        functools.partial(write_kernel, spots),
        out_shape=jax.ShapeDtypeStruct((ROWS, D), BF16),
        in_specs=[pl.BlockSpec(memory_space=pltpu.VMEM)] * n + [ANY] * len(given),
        out_specs=ANY,
        scratch_shapes=[pltpu.SemaphoreType.DMA((n, 2 * M // U))],
        input_output_aliases={n: 0} if given else {},
        compiler_params=pltpu.CompilerParams(vmem_limit_bytes=16 * 1024 * 1024),
        cost_estimate=pl.CostEstimate(flops=10**9, bytes_accessed=24 * 2**20, transcendentals=0),
        name="write",
    )(*parts, *given)


def index(x, y, core):
    return (x * 2 + y) * 2 + core


def pairs(to):
    return [(index(x, y, c), index(*to(x, y, c))) for x in (0, 1) for y in (0, 1) for c in (0, 1)]


FIRST = pairs(lambda x, y, c: (x, 1 - y, c) if c == 0 else (1 - x, y, c))
SECOND = pairs(lambda x, y, c: (1 - x, y, c) if c == 0 else (x, 1 - y, c))
SIBLING = pairs(lambda x, y, c: (x, y, 1 - c))


def solution(mesh):
    def send(value, perm):
        return lax.ppermute(value, "tp", perm)

    def step(x, dy, gate, up, w_gate, w_up, w_down):
        shard, upper, lower, d_gate, d_up, hidden, block = scatter(dy, gate, up, w_gate, w_up, w_down)
        first_a, first_b = send(upper, FIRST), send(lower, FIRST)
        second = send(shard, SECOND)
        own_twin = send(shard, SIBLING)
        both_a = send(first_a, SECOND)
        both_b, both_c = send(first_b[: M - TAIL], SECOND), send(first_b[M - TAIL :], SECOND)
        first_a_twin, first_b_twin = send(first_a, SIBLING), send(first_b, SIBLING)
        second_twin = send(second, SIBLING)
        both_a_twin, both_b_twin = send(both_a, SIBLING), send(both_b, SIBLING)
        both_c_twin = send(both_c, SIBLING)
        *wide, ahead = wide_grads(x, d_gate, d_up, 0, 3, x, 3)
        dw_gate, dw_up, ahead = wide_grads(x, d_gate, d_up, 3, 3, dy, EARLY // BN, ahead, wide)
        dw_down, dx = down_grad(
            hidden, dy, block, ahead, (shard, own_twin, first_a, first_b, second),
            ((0, 0, 0, 0, 2 * M), (1, 0, 0, 0, 2 * M), (0, 1, 0, 0, M), (0, 1, 0, M, M), (0, 0, 1, 0, 2 * M)),
        )
        dx = write(
            (first_a_twin, first_b_twin, second_twin, both_a),
            ((1, 1, 0, 0, M), (1, 1, 0, M, M), (1, 0, 1, 0, 2 * M), (0, 1, 1, 0, M)),
            dx,
        )
        dx = write((both_a_twin, both_b), ((1, 1, 1, 0, M), (0, 1, 1, M, M - TAIL)), dx)
        dx = write((both_b_twin, both_c), ((1, 1, 1, M, M - TAIL), (0, 1, 1, 2 * M - TAIL, TAIL)), dx)
        dx = write((both_c_twin,), ((1, 1, 1, 2 * M - TAIL, TAIL),), dx)
        return dx, dw_gate, dw_up, dw_down

    tokens, columns, rows = P("dp", None), P(None, "tp"), P("tp", None)
    return jax.shard_map(
        step,
        mesh=mesh,
        in_specs=(tokens, tokens, P("dp", "tp"), P("dp", "tp"), columns, columns, rows),
        out_specs=(tokens, P("dp", "tp"), P("dp", "tp"), P(("dp", "tp"), None)),
        check_vma=False,
    )
```

```python
import functools

import jax
import jax.numpy as jnp
from jax import lax
from jax.experimental import pallas as pl
from jax.experimental.pallas import tpu as pltpu
from jax.sharding import PartitionSpec as P


SCATTER_MIB, WIDE_MIB, DOWN_MIB = 44, 24, 24

BF16, F32 = jnp.bfloat16, jnp.float32
ROWS, D, FL = 2048, 3072, 1024
M = 256
TAIL = 64
U = M // 2
HALF = D // 2
W = 512
PIECES = HALF // W
BN = 512
EARLY = 3 * BN
LATE = (D - EARLY) // BN
STEPS = ROWS // M
ANY = pl.BlockSpec(memory_space=pl.ANY)


def nt(a, b):
    return lax.dot_general(a, b, (((1,), (1,)), ((), ())), preferred_element_type=F32)


def turned(a, b):
    return lax.dot_general(a, b, (((0,), (0,)), ((), ())), preferred_element_type=F32)


def places(parts, spots, out, sem):
    _, core, y, x = place()
    copies = []
    for k, (part, (twin, along_first, along_second, row, count)) in enumerate(zip(parts, spots)):
        half = core + twin - 2 * core * twin
        flip_y = along_first * (1 - half) + along_second * half
        flip_x = along_first * half + along_second * (1 - half)
        to_x, to_y = x + flip_x - 2 * x * flip_x, y + flip_y - 2 * y * flip_y
        cols = pl.ds(pl.multiple_of(half * HALF, HALF), HALF)
        run = TAIL if count % U else U
        for i in range(0, count, run):
            rows = pl.ds(pl.multiple_of((to_x * 2 + to_y) * 2 * M + row + i, run), run)
            copies.append(pltpu.make_async_copy(part.at[pl.ds(i, run)], out.at[rows, cols], sem.at[k, i // run]))
    return copies


def place():
    me = lax.axis_index("tp")
    core, y, x = me % 2, (me // 2) % 2, me // 4
    return me, core, y, x


def rows_of(p, x, y):
    diag, own = 1 - jnp.minimum(p // 2, 1), p // 6
    mid = 1 - diag - own
    at = diag * p * M + own * (p - 6) * M + mid * (p - 2) * U

    def run(flip_x, flip_y):
        to_x, to_y = x + flip_x - 2 * x * flip_x, y + flip_y - 2 * y * flip_y
        return (to_x * 2 + to_y) * 2 * M + at

    return run(diag, diag + mid), run(diag + mid, diag) + (1 - mid) * U


def scatter_kernel(
    dy, gate, up, w_gate, w_up, w_down,
    shard, upper, lower, d_gate, d_up, hidden, block,
    wide, wd, inb, dgb, dub, acc, sum_own,
    sib_out, sib_in, one_out, one_in, two_out, two_in,
    down_sem, wide_sem, in_sem, half_r,
    sib_s, sib_r, one_s, one_r, two_s, two_r,
):
    me, core, y, x = place()
    sibling = me + 1 - 2 * core
    near_x, near_y = me + 4 - 8 * x, me + 2 - 4 * y
    first = near_y * (1 - core) + near_x * core
    second = near_x * (1 - core) + near_y * core
    own_col, sib_col = core * HALF, (1 - core) * HALF

    def inputs(p, slot):
        made = []
        for h, row in enumerate(rows_of(p, x, y)):
            rows, at = pl.ds(pl.multiple_of(row, U), U), 0
            for far in (dy, gate, up):
                near = inb.at[slot, pl.ds(h * U, U), pl.ds(at, far.shape[1])]
                made.append(pltpu.make_async_copy(far.at[rows], near, in_sem.at[slot]))
                at += far.shape[1]
        return made

    def inputs_here(slot):
        pltpu.make_async_copy(inb.at[slot], inb.at[slot], in_sem.at[slot]).wait()

    def columns(base, j):
        return pl.ds(pl.multiple_of(base + j * W, 256), W)

    down = []
    for n in range(FL // 256):
        at = pl.ds(n * 256, 256)
        down.append(pltpu.make_async_copy(w_down.at[at], wd.at[at], down_sem.at[n]))
    slices = {}
    for j in range(PIECES):
        for side, base in ((0, sib_col), (1, own_col)):
            at = columns(base, j)
            slices[side, j] = [
                pltpu.make_async_copy(w.at[at], wide.at[k, at], wide_sem.at[side, j])
                for k, w in enumerate((w_gate, w_up))
            ]

    def remote(src, dst, send, recv, to):
        return pltpu.make_async_remote_copy(
            src_ref=src, dst_ref=dst, send_sem=send, recv_sem=recv,
            device_id={"tp": to}, device_id_type=pl.DeviceIdType.MESH,
        )

    def to_sibling(p, j):
        return remote(sib_out.at[p % 2, j], sib_in.at[p % 2, j], sib_s.at[p % 2], sib_r.at[p % 2, j], sibling)

    def to_first(k, j):
        return remote(one_out.at[k, j], one_in.at[k, j], one_s, one_r.at[k], first)

    def sent(p):
        remote(sib_out.at[p % 2], sib_in.at[p % 2], sib_s.at[p % 2], sib_r.at[0, 0], sibling).wait_send()

    def unit_here(into, sems, k):
        pltpu.make_async_copy(into.at[k], into.at[k], sems.at[k]).wait()

    def to_second(k, j):
        return remote(two_out.at[k, j], two_in.at[k, j], two_s, two_r.at[k], second)

    for c in inputs(0, 0) + down[:2]:
        c.start()

    barrier = pltpu.get_barrier_semaphore()
    for other in (sibling, first, second):
        pl.semaphore_signal(barrier, inc=1, device_id={"tp": other}, device_id_type=pl.DeviceIdType.MESH)
    pl.semaphore_wait(barrier, 3)
    for c in down[2:]:
        c.start()

    def keep(to, p, at, value):
        value = value.astype(BF16)
        for h, row in enumerate(rows_of(p, x, y)):
            to[pl.ds(pl.multiple_of(row, U), U), at] = value[h * U : (h + 1) * U]
        return value

    def hidden_grads(p, slot, n):
        at = slice(n * 256, (n + 1) * 256)
        d_hidden = nt(inb[slot, :, :D], wd[at, :])
        g = inb[slot, :, D + n * 256 : D + (n + 1) * 256].astype(F32)
        u = inb[slot, :, D + FL + n * 256 : D + FL + (n + 1) * 256].astype(F32)
        s = jax.nn.sigmoid(g)
        act = g * s
        keep(hidden, p, at, act * u)
        dub[:, at] = keep(d_up, p, at, d_hidden * act)
        dgb[:, at] = keep(d_gate, p, at, d_hidden * u * (s + act * (1 - s)))

    def term(base, j):
        at = columns(base, j)
        return (nt(dgb[...], wide[0, at, :]) + nt(dub[...], wide[1, at, :])).reshape(2, U, W)

    def for_sibling(p, pieces):
        for j in pieces:
            sib_out[p % 2, j] = term(sib_col, j).astype(BF16)
        for j in pieces:
            to_sibling(p, j).start()

    def chip_sum(p, j, h):
        return acc[j, h] + sib_in[p % 2, j, h].astype(F32)

    def send_diagonal(p, j):
        for h in range(2):
            one_out[2 * p + h, j] = chip_sum(p, j, h).astype(BF16)
            to_first(2 * p + h, j).start()

    def send_middle(p):
        q = p - 2
        for j in range(PIECES):
            to_sibling(p, j).wait_recv()
            one_out[4 + q, j] = chip_sum(p, j, core).astype(BF16)
            to_first(4 + q, j).start()
        unit_here(one_in, one_r, q)
        for j in range(PIECES):
            two_out[q, j] = (chip_sum(p, j, 1 - core) + one_in[q, j].astype(F32)).astype(BF16)
            to_second(q, j).start()

    def keep_own(p):
        for j in range(PIECES):
            to_sibling(p, j).wait_recv()
            for h in range(2):
                sum_own[2 * (p - 6) + h, j] = chip_sum(p, j, h)

    def diagonal_step(p, ready, done):
        for j in range(done, PIECES + 1):
            if done + (done > 0) <= j < PIECES:
                ready(0, j)
                for_sibling(p, (j,))
            if j > done:
                ready(1, j - 1)
                acc[j - 1] = term(own_col, j - 1)
                to_sibling(p, j - 1).wait_recv()
                send_diagonal(p, j - 1)

    def arrived(side, j):
        here = wide.at[:, columns((sib_col, own_col)[side], j)]
        pltpu.make_async_copy(here, here, wide_sem.at[side, j]).wait()

    down_inputs = []
    for k in range(ROWS // FL):
        near = wd.at[:, pl.ds(k * EARLY, EARLY)]
        down_inputs.append(pltpu.make_async_copy(dy.at[pl.ds(k * FL, FL), pl.ds(0, EARLY)], near, down_sem.at[k]))

    def first_piece():
        halves = [pl.ds(i * (W // 2), W // 2) for i in range(2)]

        def copy(i):
            a, b = sib_out.at[0, 0, :, :, halves[i]], sib_in.at[0, 0, :, :, halves[i]]
            return remote(a, b, sib_s.at[0], half_r.at[i], sibling)

        for i in range(2):
            for side, base in enumerate((sib_col, own_col)):
                if i == 0:
                    arrived(side, 0)
                at = pl.ds(pl.multiple_of(base + i * (W // 2), 256), W // 2)
                part = (nt(dgb[...], wide[0, at, :]) + nt(dub[...], wide[1, at, :])).reshape(2, U, W // 2)
                if side:
                    acc[0, :, :, halves[i]] = part
                else:
                    sib_out[0, 0, :, :, halves[i]] = part.astype(BF16)
                    copy(i).start()
        for i in range(2):
            copy(i).wait_recv()
            for h in range(2):
                total = acc[0, h, :, halves[i]] + sib_in[0, 0, h, :, halves[i]].astype(F32)
                one_out[h, 0, :, halves[i]] = total.astype(BF16)
                a, b = one_out.at[h, 0, :, halves[i]], one_in.at[h, 0, :, halves[i]]
                remote(a, b, one_s, one_r.at[h], first).start()
            if i == 0:
                arrived(0, 1)
                for_sibling(0, (1,))

    inputs_here(0)
    for c in down[:2]:
        c.wait()
    for c in slices[0, 0] + slices[1, 0]:
        c.start()
    for n in range(2):
        hidden_grads(0, 0, n)
    for c in down[2:]:
        c.wait()
    for k in ((0, 1), (0, 2), (1, 1), (1, 2)):
        for c in slices[k]:
            c.start()
    for c in inputs(1, 1):
        c.start()
    for n in range(2, 4):
        hidden_grads(0, 0, n)
    first_piece()
    diagonal_step(0, arrived, 1)
    inputs_here(1)
    for c in inputs(2, 0):
        c.start()
    for n in range(FL // 256):
        hidden_grads(1, 1, n)
    diagonal_step(1, lambda side, j: None, 0)

    def step(p, carry):
        slot = p % 2
        inputs_here(slot)

        @pl.when(p < STEPS - 1)
        def _():
            for c in inputs(p + 1, 1 - slot):
                c.start()

        for n in range(FL // 256):
            hidden_grads(p, slot, n)

        @pl.when(jnp.logical_and(p >= 5, p < 7))
        def _():
            send_middle(p - 1)

        @pl.when(p == 7)
        def _():
            for c in down_inputs:
                c.start()
            keep_own(6)

        sent(p)
        for_sibling(p, range(PIECES))
        for j in range(PIECES):
            acc[j] = term(own_col, j)

        @pl.when(p < 4)
        def _():
            send_middle(p)

        return carry

    lax.fori_loop(2, STEPS, step, 0)
    keep_own(STEPS - 1)

    for c in down_inputs:
        c.wait()
    for n in range(0, EARLY, 256):
        right = jnp.concatenate([wd[:, pl.ds(k * EARLY + n, 256)] for k in range(ROWS // FL)])
        block[:, pl.ds(n, 256)] = turned(hidden[...], right).astype(BF16)

    for q in range(4):
        unit_here(one_in, one_r, 4 + q)
        unit_here(two_in, two_r, q)
        for j in range(PIECES):
            total = sum_own[q, j] + one_in[4 + q, j].astype(F32) + two_in[q, j].astype(F32)
            for to, row in ((upper, lower)[q // 2], q % 2), (shard, q):
                to[pl.ds(row * U, U), pl.ds(j * W, W)] = total.astype(BF16)
    for p in (STEPS - 2, STEPS - 1):
        sent(p)
    remote(one_out, one_in, one_s, one_r.at[0], first).wait_send()
    remote(two_out, two_in, two_s, two_r.at[0], second).wait_send()


def scatter(dy, gate, up, w_gate, w_up, w_down):
    dma = pltpu.SemaphoreType.DMA
    hid, part = pltpu.VMEM((ROWS, FL), BF16), pltpu.VMEM((M, HALF), BF16)
    units = lambda n: pltpu.VMEM((n, PIECES, U, W), BF16)
    twin = pltpu.VMEM((2, PIECES, 2, U, W), BF16)
    return pl.pallas_call(
        scatter_kernel,
        out_shape=(pltpu.VMEM((2 * M, HALF), BF16), part, part, hid, hid, hid, pltpu.VMEM((FL, EARLY), BF16)),
        in_specs=[ANY] * 6,
        out_specs=(pl.BlockSpec(memory_space=pltpu.VMEM),) * 7,
        scratch_shapes=[
            pltpu.VMEM((2, D, FL), BF16), pltpu.VMEM((FL, D), BF16), pltpu.VMEM((2, M, D + 2 * FL), BF16),
            pltpu.VMEM((M, FL), BF16), pltpu.VMEM((M, FL), BF16),
            pltpu.VMEM((PIECES, 2, U, W), F32), pltpu.VMEM((4, PIECES, U, W), F32),
            twin, twin, units(8), units(8), units(4), units(4),
            dma((FL // 256,)), dma((2, PIECES)), dma((2,)), dma((2,)),
            dma((2,)), dma((2, PIECES)), dma, dma((8,)), dma, dma((4,)),
        ],
        compiler_params=pltpu.CompilerParams(
            collective_id=0, has_side_effects=True, vmem_limit_bytes=SCATTER_MIB * 2**20
        ),
        cost_estimate=pl.CostEstimate(
            flops=6 * ROWS * D * FL, bytes_accessed=60 * 2**20, transcendentals=2 * ROWS * FL
        ),
        name="scatter",
    )(dy, gate, up, w_gate, w_up, w_down)


def placed(value, space):
    return pltpu.with_memory_space_constraint(value, space)


def streamed(far, near, sem, start, first, use):
    step, count = pl.program_id(0), pl.num_programs(0)

    def fetch(i):
        cols = pl.ds(pl.multiple_of((start + i) * BN, BN), BN)
        return pltpu.make_async_copy(far.at[:, cols], near.at[i % 2], sem.at[i % 2])

    if first is None:

        @pl.when(step == 0)
        def _():
            fetch(0).start()

        fetch(step).wait()

    @pl.when(step + 1 < count)
    def _():
        fetch(step + 1).start()

    if first is None:
        use(near.at[step % 2])
    else:

        @pl.when(step == 0)
        def _():
            use(first)

        @pl.when(step > 0)
        def _():
            fetch(step).wait()
            use(near.at[step % 2])


def wide_kernel(start, after, given, x, d_gate, d_up, further, *refs):
    first = refs[0] if given else None
    dw_gate, dw_up, ahead, near, sem, ahead_sem = refs[-6:]
    step, last = pl.program_id(0), pl.num_programs(0) - 1
    fetch = pltpu.make_async_copy(further.at[:, pl.ds(after * BN, BN)], ahead, ahead_sem)

    def use(block):
        xt = block[...].T
        dw_gate[...] = jnp.dot(xt, d_gate[...], preferred_element_type=F32).astype(BF16)
        dw_up[...] = jnp.dot(xt, d_up[...], preferred_element_type=F32).astype(BF16)

    streamed(x, near, sem, start, first, use)

    @pl.when(step == 0)
    def _():
        fetch.start()

    @pl.when(step == last)
    def _():
        fetch.wait()


def wide_grads(x, d_gate, d_up, start, count, further, after, first=None, into=()):
    whole = pl.BlockSpec((ROWS, FL), lambda i: (0, 0), pipeline_mode=pl.Buffered(1))
    block = pl.BlockSpec((ROWS, BN), lambda i: (0, 0), pipeline_mode=pl.Buffered(1))
    out = pl.BlockSpec((BN, FL), lambda i: (start + i, 0))
    shape = jax.ShapeDtypeStruct((D, FL), BF16)
    dma = pltpu.SemaphoreType.DMA
    given = () if first is None else (placed(first, pltpu.VMEM),)
    return pl.pallas_call(
        functools.partial(wide_kernel, start, after, bool(given)),
        grid=(count,),
        out_shape=(shape, shape, pltpu.VMEM((ROWS, BN), BF16)),
        in_specs=[ANY, whole, whole, ANY] + [block] * len(given) + [ANY] * len(into),
        out_specs=(out, out, ANY),
        scratch_shapes=[pltpu.VMEM((2, ROWS, BN), BF16), dma((2,)), dma],
        input_output_aliases={4 + len(given) + k: k for k in range(len(into))},
        compiler_params=pltpu.CompilerParams(vmem_limit_bytes=WIDE_MIB * 2**20),
        cost_estimate=pl.CostEstimate(flops=4 * ROWS * BN * count * FL, bytes_accessed=20 * 2**20, transcendentals=0),
        name="wide_grads",
    )(
        placed(x, pltpu.HBM), placed(d_gate, pltpu.VMEM), placed(d_up, pltpu.VMEM), placed(further, pltpu.HBM),
        *given, *into,
    )


def down_kernel(spots, hidden, dy, block, first, *refs):
    n = len(spots)
    parts, (out, dx, made, near, part_sem, block_sem, made_sem, sem) = refs[:n], refs[n:]
    step, last = pl.program_id(0), pl.num_programs(0) - 1

    def save(i):
        cols = pl.ds(pl.multiple_of(EARLY + i * BN, BN), BN)
        return pltpu.make_async_copy(made.at[i % 2], out.at[:, cols], made_sem.at[i % 2])

    early = pltpu.make_async_copy(block, out.at[:, pl.ds(0, EARLY)], block_sem)

    @pl.when(step >= 2)
    def _():
        save(step - 2).wait()

    def use(right):
        made[step % 2] = turned(hidden[...], right[...]).astype(BF16)

    streamed(dy, near, sem, EARLY // BN, first, use)
    save(step).start()

    @pl.when(step == 0)
    def _():
        early.start()
        for c in places(parts, spots, dx, part_sem):
            c.start()

    @pl.when(step == last)
    def _():
        early.wait()
        for c in places(parts, spots, dx, part_sem):
            c.wait()
        save(step - 1).wait()
        save(step).wait()


def down_grad(hidden, dy, block, first, parts, spots):
    n = len(parts)
    dma = pltpu.SemaphoreType.DMA
    whole = lambda *shape: pl.BlockSpec(shape, lambda i: (0, 0), pipeline_mode=pl.Buffered(1))
    return pl.pallas_call(
        functools.partial(down_kernel, spots),
        grid=(LATE,),
        out_shape=(jax.ShapeDtypeStruct((FL, D), BF16), jax.ShapeDtypeStruct((ROWS, D), BF16)),
        in_specs=[whole(ROWS, FL), ANY, whole(FL, EARLY), whole(ROWS, BN)] + [ANY] * n,
        out_specs=(ANY, ANY),
        scratch_shapes=[
            pltpu.VMEM((2, FL, BN), BF16), pltpu.VMEM((2, ROWS, BN), BF16),
            dma((n, 2 * M // U)), dma, dma((2,)), dma((2,)),
        ],
        compiler_params=pltpu.CompilerParams(vmem_limit_bytes=DOWN_MIB * 2**20),
        cost_estimate=pl.CostEstimate(flops=2 * ROWS * D * FL, bytes_accessed=24 * 2**20, transcendentals=0),
        name="down_grad",
    )(
        placed(hidden, pltpu.VMEM), placed(dy, pltpu.HBM), placed(block, pltpu.VMEM), placed(first, pltpu.VMEM),
        *parts,
    )


def write_kernel(spots, *refs):
    copies = places(refs[: len(spots)], spots, refs[-2], refs[-1])
    for c in copies:
        c.start()
    for c in copies:
        c.wait()


def write(parts, spots, into=None):
    n = len(parts)
    given = () if into is None else (into,)
    return pl.pallas_call(
        functools.partial(write_kernel, spots),
        out_shape=jax.ShapeDtypeStruct((ROWS, D), BF16),
        in_specs=[pl.BlockSpec(memory_space=pltpu.VMEM)] * n + [ANY] * len(given),
        out_specs=ANY,
        scratch_shapes=[pltpu.SemaphoreType.DMA((n, 2 * M // U))],
        input_output_aliases={n: 0} if given else {},
        compiler_params=pltpu.CompilerParams(vmem_limit_bytes=16 * 1024 * 1024),
        cost_estimate=pl.CostEstimate(flops=10**9, bytes_accessed=24 * 2**20, transcendentals=0),
        name="write",
    )(*parts, *given)


def index(x, y, core):
    return (x * 2 + y) * 2 + core


def pairs(to):
    return [(index(x, y, c), index(*to(x, y, c))) for x in (0, 1) for y in (0, 1) for c in (0, 1)]


FIRST = pairs(lambda x, y, c: (x, 1 - y, c) if c == 0 else (1 - x, y, c))
SECOND = pairs(lambda x, y, c: (1 - x, y, c) if c == 0 else (x, 1 - y, c))
SIBLING = pairs(lambda x, y, c: (x, y, 1 - c))


def solution(mesh):
    def send(value, perm):
        return lax.ppermute(value, "tp", perm)

    def step(x, dy, gate, up, w_gate, w_up, w_down):
        shard, upper, lower, d_gate, d_up, hidden, block = scatter(dy, gate, up, w_gate, w_up, w_down)
        first_a, first_b = send(upper, FIRST), send(lower, FIRST)
        second = send(shard, SECOND)
        own_twin = send(shard, SIBLING)
        both_a = send(first_a, SECOND)
        both_b, both_c = send(first_b[: M - TAIL], SECOND), send(first_b[M - TAIL :], SECOND)
        first_a_twin, first_b_twin = send(first_a, SIBLING), send(first_b, SIBLING)
        second_twin = send(second, SIBLING)
        both_a_twin, both_b_twin = send(both_a, SIBLING), send(both_b, SIBLING)
        both_c_twin = send(both_c, SIBLING)
        *wide, ahead = wide_grads(x, d_gate, d_up, 0, 3, x, 3)
        dw_gate, dw_up, ahead = wide_grads(x, d_gate, d_up, 3, 3, dy, EARLY // BN, ahead, wide)
        dw_down, dx = down_grad(
            hidden, dy, block, ahead, (shard, own_twin, first_a, first_b, second),
            ((0, 0, 0, 0, 2 * M), (1, 0, 0, 0, 2 * M), (0, 1, 0, 0, M), (0, 1, 0, M, M), (0, 0, 1, 0, 2 * M)),
        )
        dx = write(
            (first_a_twin, first_b_twin, second_twin, both_a),
            ((1, 1, 0, 0, M), (1, 1, 0, M, M), (1, 0, 1, 0, 2 * M), (0, 1, 1, 0, M)),
            dx,
        )
        dx = write((both_a_twin, both_b), ((1, 1, 1, 0, M), (0, 1, 1, M, M - TAIL)), dx)
        dx = write((both_b_twin, both_c), ((1, 1, 1, M, M - TAIL), (0, 1, 1, 2 * M - TAIL, TAIL)), dx)
        dx = write((both_c_twin,), ((1, 1, 1, 2 * M - TAIL, TAIL),), dx)
        return dx, dw_gate, dw_up, dw_down

    tokens, columns, rows = P("dp", None), P(None, "tp"), P("tp", None)
    return jax.shard_map(
        step,
        mesh=mesh,
        in_specs=(tokens, tokens, P("dp", "tp"), P("dp", "tp"), columns, columns, rows),
        out_specs=(tokens, P("dp", "tp"), P("dp", "tp"), P(("dp", "tp"), None)),
        check_vma=False,
    )
```
